32 devices in a mesh: groups: 2 (over y), fld: 8 (over z, x), rep: 2 (over core).
Axes of the slice: x: 2, y: 2, z: 4, core: 2. Of those that a mesh axis runs over, the one named last changes fastest.
Arguments:
- feature_ids: int32 [4096, 40], P('groups', 'fld'), parts along dimension 0, may hold values from 0 to 65535, as said below
- field_slot: int32 [40], replicated, may hold values from 0 to 39, as said below
- table: bfloat16 [2621440, 64], P(('fld', 'rep')), may hold values from -48 to 48
- query_weight: bfloat16 [2, 64, 64], replicated, may hold values from -0.75 to 0.75
- key_weight: bfloat16 [2, 64, 64], replicated, may hold values from -0.75 to 0.75
- value_weight: bfloat16 [2, 64, 64], replicated, may hold values from -0.75 to 0.75
- residual_weight: bfloat16 [2, 64, 64], replicated, may hold values from -0.75 to 0.75
- out_weight: float32 [40, 64], replicated, may hold values from -0.125 to 0.125
Outputs:
- interacted: bfloat16 [40, 4096, 64], P('fld', ('groups', 'rep')), parts along dimension 1
- logits: float32 [2, 2048], P('rep', ('groups', 'fld')), parts along dimension 1
The draws below stay inside these ranges and needn't reach their ends.
There are 2 independent parts, one for each index of `groups`. The reference program is written for one: setup_inputs(seed, part) draws one part's arguments, and reference() takes and returns one part's arrays. A program takes and returns all parts, laid end to end along the dimension named above; an argument that names none is the same for every part. Nothing has to cross between parts.
Inputs may be any that keep to these rules, and one draw needn't show every extreme that they name: `feature_ids`: in each column the ids lie below a table size of that slot, which differs from slot to slot. `field_slot`: distinct slots.
All inputs are finite; a program needn't handle non-finite values.
Results may differ from the reference program's by a relative error of at most 0.006.
The reference program's roundings to bfloat16 on the way count: a program that leaves them out, or rounds other values in their place, can miss the bound.
Values may be sent and summed in bfloat16 or wider, within the bound.
No kernel may reach another device: no remote copies, remote signals or barrier semaphores. Data moves between devices by JAX's collectives and lax.ppermute only.
A program may use at most 128 MiB of HBM per device.

```python
import jax
import jax.numpy as jnp
from jax import lax

FEATURE_FIELDS = 40
WIDTH = 64
HEADS = 2
ROWS_SLOT = 65536
LAYERS = 2
EX_DEV = 128
SLOTS = 40
EXAMPLES = 2048
N_REP = 2


def draw_feature_ids(key, part):
    size_key = jax.random.fold_in(key, 11)
    id_key = jax.random.fold_in(key, 12)
    table_sizes = jax.random.randint(size_key, (1, SLOTS), ROWS_SLOT // 8, ROWS_SLOT + 1)
    return jax.random.randint(id_key, (EXAMPLES, SLOTS), 0, table_sizes).astype(jnp.int32)


def draw_field_slot(key, part):
    order_key = jax.random.fold_in(key, 31)
    return jax.random.permutation(order_key, SLOTS)[:FEATURE_FIELDS].astype(jnp.int32)


def draw_table(key, part):
    normal_values = jax.random.normal(jax.random.fold_in(key, 21), (SLOTS * ROWS_SLOT, WIDTH), jnp.float32)
    return jnp.clip(normal_values, -4.0, 4.0).astype(jnp.bfloat16)


def bell_draw(key, shape, deviation, reach, kind=jnp.bfloat16):
    entries = jax.random.normal(key, shape, jnp.float32) * deviation
    return jnp.minimum(jnp.maximum(entries, -reach), reach).astype(kind)


def setup_inputs(seed: int = 0, part: int = 0) -> dict:
    key_of = jax.random.split(jax.random.key(seed), 9)
    own_keys = jax.random.split(jax.random.fold_in(key_of[8], part), 9)
    feature_ids = draw_feature_ids(jax.random.fold_in(jax.random.fold_in(key_of[8], part), 71), part)
    field_slot = draw_field_slot(jax.random.fold_in(key_of[8], 71), part)
    table = draw_table(jax.random.fold_in(key_of[8], 71), part)
    query_weight = bell_draw(key_of[3], (LAYERS, WIDTH, WIDTH), WIDTH ** -0.5, 0.75)
    key_weight = bell_draw(key_of[4], (LAYERS, WIDTH, WIDTH), WIDTH ** -0.5, 0.75)
    value_weight = bell_draw(key_of[5], (LAYERS, WIDTH, WIDTH), WIDTH ** -0.5, 0.75)
    residual_weight = bell_draw(key_of[6], (LAYERS, WIDTH, WIDTH), WIDTH ** -0.5, 0.75)
    out_weight = bell_draw(key_of[7], (FEATURE_FIELDS, WIDTH), (FEATURE_FIELDS * WIDTH) ** -0.5, 0.125, jnp.float32)
    return dict(feature_ids=feature_ids, field_slot=field_slot, table=table, query_weight=query_weight, key_weight=key_weight, value_weight=value_weight, residual_weight=residual_weight, out_weight=out_weight)


def rounded(values):
    return lax.optimization_barrier(values.astype(jnp.bfloat16)).astype(jnp.float32)

def attend(layer_in, w_query, w_key, w_value, w_skip, head_count):
    batch_rows, field_count, width = layer_in.shape
    head_size = width // head_count
    source = layer_in.astype(jnp.float32)

    def project(weight):
        return jnp.einsum('nfe,ed->nfd', source, weight.astype(jnp.float32))
    query_rows = rounded(project(w_query)).reshape(batch_rows, field_count, head_count, head_size)
    matches = rounded(project(w_key)).reshape(batch_rows, field_count, head_count, head_size)
    contents = rounded(project(w_value)).reshape(batch_rows, field_count, head_count, head_size)
    skip_output = project(w_skip)
    scores = jnp.einsum('nfhd,nghd->nhfg', query_rows, matches) / jnp.sqrt(jnp.float32(head_size))
    attention = rounded(jax.nn.softmax(scores, axis=-1))
    mixed = jnp.einsum('nhfg,nghd->nfhd', attention, contents).reshape(batch_rows, field_count, width)
    return jax.nn.relu(mixed + skip_output).astype(jnp.bfloat16)

def reference(feature_ids, field_slot, table, query_weight, key_weight, value_weight, residual_weight, out_weight):
    slot_range = jnp.arange(SLOTS, dtype=jnp.int32)
    select_mask = (field_slot[:, None] == slot_range[None, :]).astype(jnp.float32)
    blocks = feature_ids.reshape(EXAMPLES // EX_DEV, EX_DEV, SLOTS)

    def one_block(block_ids):
        row_index = block_ids + (slot_range * ROWS_SLOT)[None, :]
        looked = jnp.take(table, row_index, axis=0).astype(jnp.float32)
        layer_in = jnp.einsum('nse,fs->nfe', looked, select_mask).astype(jnp.bfloat16)
        for layer in range(LAYERS):
            layer_in = attend(layer_in, query_weight[layer], key_weight[layer], value_weight[layer], residual_weight[layer], HEADS)
        hidden_state = layer_in.astype(jnp.float32)
        logit_rows = jnp.einsum('nfd,fd->n', hidden_state, out_weight, precision=lax.Precision.HIGHEST)
        placed = jnp.einsum('nfd,fs->snd', hidden_state, select_mask).astype(jnp.bfloat16)
        return (placed, logit_rows)
    placed, logit_rows = lax.map(one_block, blocks)
    interacted = jnp.transpose(placed, (1, 0, 2, 3)).reshape(SLOTS, EXAMPLES, WIDTH)
    logits = logit_rows.reshape(N_REP, EXAMPLES // N_REP)
    return (interacted, logits)
```

```python
import functools
import math

import jax
import jax.numpy as jnp
from jax import lax
from jax.experimental import pallas as pl
from jax.experimental.pallas import tpu as pltpu
from jax.sharding import PartitionSpec as P

HEADS = 2
F32 = jnp.float32
BF16 = jnp.bfloat16
LANES = 128
VMEM_BYTES = 60000 * 1024


def divisor(count, options):
    return next(c for c in options if count % c == 0)


def lookup_kernel(code_ref, ends_ref, tab_ref, out_ref, tab, sem, *, chunks, unroll):
    owned = tab_ref.shape[1]
    blocks, slots, width, lanes = out_ref.shape
    step = owned // chunks

    def fetch(c):
        at = pl.ds(c * step, step)
        return pltpu.make_async_copy(tab_ref.at[:, at], tab.at[:, at], sem.at[c])

    for c in range(chunks):
        fetch(c).start()
    tab[:, pl.ds(owned, lanes)] = jnp.zeros((width, lanes), tab.dtype)
    lane = lax.broadcasted_iota(jnp.int32, (width, lanes), 1)
    for j in range(slots):
        low = ends_ref[j - 1] if j else 0
        high = ends_ref[j]
        for c in range(chunks):

            @pl.when((c >= low) & (c < high))
            def _():
                fetch(c).wait()

        def block(b, carry, j=j):
            base = (j * blocks + b) * lanes

            def some(i, acc):
                for u in range(unroll):
                    k = i * unroll + u
                    code = code_ref[base + k]
                    start = pl.multiple_of((code >> 7) * LANES, LANES)
                    found = pltpu.roll(tab[:, pl.ds(start, lanes)], code & (LANES - 1), 1)
                    acc = jnp.where(lane == k, found, acc)
                return acc

            acc = lax.fori_loop(0, lanes // unroll, some, jnp.zeros((width, lanes), tab.dtype))
            out_ref[b, j] = acc
            return carry

        lax.fori_loop(0, blocks, block, 0)


def lookup(code, ends, table_t, blocks, slots):
    width, owned = table_t.shape
    chunks = divisor(owned // LANES, (10, 8, 5, 4, 2, 1))
    return pl.pallas_call(
        functools.partial(lookup_kernel, chunks=chunks, unroll=64),
        out_shape=jax.ShapeDtypeStruct((blocks, slots, width, LANES), BF16),
        in_specs=[
            pl.BlockSpec(memory_space=pltpu.SMEM),
            pl.BlockSpec(memory_space=pltpu.SMEM),
            pl.BlockSpec(memory_space=pl.ANY),
        ],
        out_specs=pl.BlockSpec(memory_space=pltpu.VMEM),
        scratch_shapes=[
            pltpu.VMEM((width, owned + LANES), BF16),
            pltpu.SemaphoreType.DMA((chunks,)),
        ],
        compiler_params=pltpu.CompilerParams(vmem_limit_bytes=VMEM_BYTES),
    )(code, ends, table_t)


def project(load, w, q_s, k_s, v_s, r_s, fields, width, lanes):
    def pair(i, carry):
        f = 2 * i
        x2 = jnp.concatenate([load(f), load(f + 1)], axis=1)
        y = lax.dot_general(w, x2, (((1,), (0,)), ((), ())), preferred_element_type=F32)
        for u in range(2):
            yu = y[:, u * lanes : (u + 1) * lanes]
            qkv = yu[: 3 * width].astype(BF16).astype(F32)
            q_s[f + u] = qkv[:width]
            k_s[pl.ds(f + u, width, stride=fields), :] = qkv[width : 2 * width]
            v_s[f + u] = qkv[2 * width :]
            r_s[f + u] = yu[3 * width :]
        return carry

    lax.fori_loop(0, fields // 2, pair, 0)


def attend(q_s, k_s, v_s, r_s, a_s, store, fields, width, lanes, group):
    size = width // HEADS
    scale = math.log2(math.e) / math.sqrt(size)

    def some(i, carry):
        f0 = i * group
        for h in range(HEADS):
            scores = [None] * group
            for d in range(size):
                row = h * size + d
                match = k_s[row * fields : (row + 1) * fields, :]
                for u in range(group):
                    term = match * q_s[f0 + u, pl.ds(row, 1), :]
                    scores[u] = term if scores[u] is None else scores[u] + term
            for u in range(group):
                top = jnp.max(scores[u], axis=0, keepdims=True)
                e = jnp.exp2((scores[u] - top) * scale)
                total = jnp.sum(e, axis=0, keepdims=True)
                a_s[u * fields : (u + 1) * fields, :] = (e / total).astype(BF16).astype(F32)
            mixed = [None] * group
            for g in range(fields):
                content = v_s[g, h * size : (h + 1) * size, :]
                for u in range(group):
                    term = content * a_s[u * fields + g : u * fields + g + 1, :]
                    mixed[u] = term if mixed[u] is None else mixed[u] + term
            for u in range(group):
                out = mixed[u] + r_s[f0 + u, h * size : (h + 1) * size, :]
                store(f0 + u, h * size, jnp.maximum(out, 0.0).astype(BF16))
        return carry

    lax.fori_loop(0, fields // group, some, 0)


def interact_kernel(
    place_ref, x_ref, wq_ref, wk_ref, wv_ref, wr_ref, o_ref, x_s, h_s, q_s, k_s, v_s, r_s, a_s, *, sources, group
):
    slots, width, lanes = o_ref.shape
    fields = h_s.shape[0]
    layers = wq_ref.shape[0]
    size = width // HEADS
    per = len(sources)

    def gather(i, carry):
        for local, parts in enumerate(sources):
            found = None
            for r, j in parts:
                part = x_ref[i, r, j]
                found = part if found is None else found + part
            x_s[i * per + local] = found
        return carry

    lax.fori_loop(0, slots // per, gather, 0)
    whole = slots == fields

    def slot(f):
        return f if whole else place_ref[f]

    if not whole:

        def clear(s, carry):
            o_ref[s] = jnp.zeros((width, lanes), BF16)
            return carry

        lax.fori_loop(0, slots, clear, 0)
    for l in range(layers):
        w = jnp.concatenate(
            [ref[l].astype(F32).T.astype(BF16) for ref in (wq_ref, wk_ref, wv_ref, wr_ref)], axis=0
        )
        load = (lambda f: x_s[slot(f)]) if l == 0 else (lambda f: h_s[f])
        project(load, w, q_s, k_s, v_s, r_s, fields, width, lanes)

        def store(f, at, out, last=l == layers - 1):
            if last:
                o_ref[slot(f), at : at + size, :] = out
            else:
                h_s[f, at : at + size, :] = out

        attend(q_s, k_s, v_s, r_s, a_s, store, fields, width, lanes, group)


def interact(place, arrived, weights, sources, fields):
    chips, reps, held, width, lanes = arrived.shape
    slots = chips * len(sources)
    group = divisor(fields, (4, 2, 1))
    wide = pltpu.VMEM((fields, width, lanes), F32)
    vmem = pl.BlockSpec(memory_space=pltpu.VMEM)
    return pl.pallas_call(
        functools.partial(interact_kernel, sources=sources, group=group),
        out_shape=jax.ShapeDtypeStruct((slots, width, lanes), BF16),
        in_specs=[pl.BlockSpec(memory_space=pltpu.SMEM)] + [vmem] * 5,
        out_specs=vmem,
        scratch_shapes=[
            pltpu.VMEM((slots, width, lanes), BF16),
            pltpu.VMEM((fields, width, lanes), BF16),
            wide,
            pltpu.VMEM((width * fields, lanes), F32),
            wide,
            wide,
            pltpu.VMEM((group * fields, lanes), F32),
        ],
        compiler_params=pltpu.CompilerParams(vmem_limit_bytes=VMEM_BYTES),
    )(place, arrived, *weights)


def per_device(
    feature_ids,
    field_slot,
    table,
    query_weight,
    key_weight,
    value_weight,
    residual_weight,
    out_weight,
):
    total, per = feature_ids.shape
    owned, width = table.shape
    chips = lax.axis_size("fld")
    reps = lax.axis_size("rep")
    rep = lax.axis_index("rep")
    half = total // reps
    peer = half // chips
    blocks = chips * reps
    rows_slot = owned * reps // per
    slot_count = chips * per
    fields = field_slot.shape[0]

    spans = [(r * owned // rows_slot, -(-(r + 1) * owned // rows_slot)) for r in range(reps)]
    held = max(b - a for a, b in spans)
    firsts = [min(a, per - held) for a, _ in spans]
    sources = tuple(
        tuple((r, s - firsts[r]) for r in range(reps) if spans[r][0] <= s < spans[r][1])
        for s in range(per)
    )
    chunks = divisor(owned // LANES, (10, 8, 5, 4, 2, 1))
    step = owned // chunks
    first = jnp.asarray(firsts, jnp.int32)[rep]
    ends = [
        [min(chunks, -(-((firsts[r] + j + 1) * rows_slot - r * owned) // step)) for j in range(held)]
        for r in range(reps)
    ]
    ends = jnp.asarray(ends, jnp.int32)[rep]

    ids = lax.dynamic_slice_in_dim(jnp.transpose(feature_ids), first, held, 0)
    rows = ids + (first + jnp.arange(held, dtype=jnp.int32))[:, None] * rows_slot - rep * owned
    rows = jnp.where((rows >= 0) & (rows < owned), rows, owned)
    rows = rows.reshape(held, reps, chips, peer).transpose(0, 2, 1, 3).reshape(held, total)
    place = jnp.arange(total, dtype=jnp.int32) & (LANES - 1)
    code = (rows & ~(LANES - 1)) | ((place - rows) & (LANES - 1))

    found = lookup(code.reshape(-1), ends, jnp.transpose(table), blocks, held)
    arrived = lax.all_to_all(found, ("fld", "rep"), 0, 0, tiled=True)
    arrived = arrived.reshape(chips, reps, held, width, peer)
    weights = (query_weight, key_weight, value_weight, residual_weight)
    hidden = interact(field_slot, arrived, weights, sources, fields)

    sent = lax.all_to_all(hidden, "fld", 0, 0, tiled=True)
    select = (field_slot[:, None] == jnp.arange(slot_count, dtype=jnp.int32)[None, :]).astype(F32)
    slot_weight = jnp.einsum("fs,fd->sd", select, out_weight, precision=lax.Precision.HIGHEST)
    logits = jnp.einsum(
        "sdn,sd->n", hidden.astype(F32), slot_weight, precision=lax.Precision.HIGHEST
    )
    interacted = (
        sent.reshape(chips, per, width, peer).transpose(1, 0, 3, 2).reshape(per, half, width)
    )
    return (interacted, logits.reshape(1, peer))


def solution(mesh):
    placed = (P("groups", "fld"), P(), P(("fld", "rep"), None), P(), P(), P(), P(), P())
    return jax.shard_map(
        per_device,
        mesh=mesh,
        in_specs=placed,
        out_specs=(P("fld", ("groups", "rep"), None), P("rep", ("groups", "fld"))),
        check_vma=False,
    )
```

```python
import functools
import math

import jax
import jax.numpy as jnp
from jax import lax
from jax.experimental import pallas as pl
from jax.experimental.pallas import tpu as pltpu
from jax.sharding import PartitionSpec as P

HEADS = 2
F32 = jnp.float32
BF16 = jnp.bfloat16
LANES = 128
VMEM_BYTES = 58 * 1024 * 1024


def divisor(count, options):
    return next(c for c in options if count % c == 0)


def by_rep(options):
    rep = lax.axis_index("rep")
    found = jnp.int32(options[0])
    for r, option in enumerate(options[1:], 1):
        found = jnp.where(rep == r, jnp.int32(option), found)
    return found


def lookup_kernel(
    ids_ref, tab_ref, *refs, step, slot_of, shift_of, bounds_of, owned
):
    out_ref, land, tab, stage, lines, odd_ref, row_ref, sem, row_sem = refs[-9:]
    blocks, slots, width, lanes = out_ref.shape
    reps = len(bounds_of[0])
    rep = lax.axis_index("rep")
    buffers = land.shape[0]
    batch = stage.shape[0] // lanes
    spare = tab.shape[0] - 8
    bounds = [by_rep(b) for b in bounds_of]
    first, last = bounds[0], bounds[-1]
    pairs = step // (2 * lanes)

    def fetch(c):
        b = lax.rem(c, buffers)
        at = pl.ds(pl.multiple_of(c * step, step), step)
        return pltpu.make_async_copy(tab_ref.at[:, at], land.at[b], sem.at[b])

    for i in range(buffers):

        @pl.when(first + i < last)
        def _():
            fetch(first + i).start()

    tab[pl.ds(spare, 8), :] = jnp.zeros((8, 2 * width), F32)
    for j in range(slots):
        shift = by_rep(shift_of[j])
        for b in range(blocks):
            at = ((b % reps) * (blocks // reps) + b // reps) * lanes
            rows = ids_ref[slot_of[j][0] : slot_of[j][0] + 1, at : at + lanes]
            for r, slot in enumerate(slot_of[j][1:], 1):
                rows = jnp.where(rep == r, ids_ref[slot : slot + 1, at : at + lanes], rows)
            rows = rows + shift
            here = (rows >= 0) & (rows < owned)
            rows = rows - first * step
            line = ((rows >> 8) << 7) | (rows & (lanes - 1))
            lines[pl.ds(j * blocks + b, 1), :] = jnp.where(here, line, spare)
            odd_ref[pl.ds(j * blocks + b, 1), :] = (rows >> 7) & 1
    rows_copy = pltpu.make_async_copy(lines, row_ref, row_sem)
    rows_copy.start()
    rows_copy.wait()
    for j in range(slots):

        def chunk(c, carry):
            fetch(c).wait()
            b = lax.rem(c, buffers)

            def turn(p, carry):
                at = pl.multiple_of(p * (2 * lanes), 2 * lanes)
                two = jnp.concatenate(
                    [land[b, :, pl.ds(at, lanes)], land[b, :, pl.ds(at + lanes, lanes)]], axis=0
                )
                to = pl.multiple_of((c - first) * (step // 2) + p * lanes, lanes)
                tab[pl.ds(to, lanes), :] = two.T.astype(F32)
                return carry

            lax.fori_loop(0, pairs, turn, 0, unroll=min(pairs, 64))

            @pl.when(c + buffers < last)
            def _():
                fetch(c + buffers).start()

            return carry

        lax.fori_loop(bounds[j], bounds[j + 1], chunk, 0)

        def some_blocks(i, carry, j=j):
            def some(n, carry):
                at = j * blocks + i * batch + n
                to = n * lanes
                for u in range(lanes):
                    stage[pl.ds(to + u, 1), :] = tab[pl.ds(row_ref[at, u], 1), :]
                return carry

            lax.fori_loop(0, batch, some, 0)
            for g in range(batch):
                b = i * batch + g
                turned = stage[g * lanes : (g + 1) * lanes].astype(BF16).T.astype(F32)
                odd = odd_ref[pl.ds(j * blocks + b, 1), :] > 0
                out_ref[b, j] = jnp.where(odd, turned[width:], turned[:width]).astype(BF16)
            return carry

        lax.fori_loop(0, blocks // batch, some_blocks, 0)


def lookup(ids, table_t, blocks, slot_of, shift_of, bounds_of, step, most):
    width, owned = table_t.shape
    slots = len(slot_of)
    buffers = min(4, owned // step)
    batch = divisor(blocks, (4, 2, 1))
    vmem = pl.BlockSpec(memory_space=pltpu.VMEM)
    anywhere = pl.BlockSpec(memory_space=pl.ANY)
    return pl.pallas_call(
        functools.partial(
            lookup_kernel,
            step=step,
            slot_of=slot_of,
            shift_of=shift_of,
            bounds_of=bounds_of,
            owned=owned,
        ),
        out_shape=jax.ShapeDtypeStruct((blocks, slots, width, LANES), BF16),
        in_specs=[vmem, anywhere],
        out_specs=vmem,
        scratch_shapes=[
            pltpu.VMEM((buffers, width, step), BF16),
            pltpu.VMEM((most // 2 + 8, 2 * width), F32),
            pltpu.VMEM((batch * LANES, 2 * width), F32),
            pltpu.VMEM((slots * blocks, LANES), jnp.int32),
            pltpu.VMEM((slots * blocks, LANES), jnp.int32),
            pltpu.SMEM((slots * blocks, LANES), jnp.int32),
            pltpu.SemaphoreType.DMA((buffers,)),
            pltpu.SemaphoreType.DMA,
        ],
        compiler_params=pltpu.CompilerParams(vmem_limit_bytes=VMEM_BYTES),
        cost_estimate=pl.CostEstimate(
            flops=slots * 12_000_000_000, bytes_accessed=2 * most * width, transcendentals=0
        ),
    )(ids, table_t)


def project(load, w, q_s, k_s, v_s, r_s, fields, width, lanes):
    def pair(i, carry):
        f = 2 * i
        x2 = jnp.concatenate([load(f), load(f + 1)], axis=1)
        y = lax.dot_general(w, x2, (((1,), (0,)), ((), ())), preferred_element_type=F32)
        for u in range(2):
            yu = y[:, u * lanes : (u + 1) * lanes]
            qkv = yu[: 3 * width].astype(BF16).astype(F32)
            q_s[f + u] = qkv[:width]
            k_s[pl.ds(f + u, width, stride=fields), :] = qkv[width : 2 * width]
            v_s[f + u] = qkv[2 * width :]
            r_s[f + u] = yu[3 * width :]
        return carry

    lax.fori_loop(0, fields // 2, pair, 0)


def attend(q_s, k_s, v_s, r_s, a_s, store, field_of, count, fields, width, group):
    size = width // HEADS
    scale = math.log2(math.e) / math.sqrt(size)

    def some(i, carry):
        own = [field_of(i * group + u) for u in range(group)]
        for h in range(HEADS):
            scores = [None] * group
            for d in range(size):
                row = h * size + d
                match = k_s[row * fields : (row + 1) * fields, :]
                for u in range(group):
                    term = match * q_s[own[u], pl.ds(row, 1), :]
                    scores[u] = term if scores[u] is None else scores[u] + term
            for u in range(group):
                top = jnp.max(scores[u], axis=0, keepdims=True)
                e = jnp.exp2((scores[u] - top) * scale)
                total = jnp.sum(e, axis=0, keepdims=True)
                a_s[u * fields : (u + 1) * fields, :] = (e / total).astype(BF16).astype(F32)
            mixed = [None] * group
            for g in range(fields):
                content = v_s[g, h * size : (h + 1) * size, :]
                for u in range(group):
                    term = content * a_s[u * fields + g : u * fields + g + 1, :]
                    mixed[u] = term if mixed[u] is None else mixed[u] + term
            for u in range(group):
                out = mixed[u] + r_s[own[u], h * size : (h + 1) * size, :]
                store(i * group + u, h * size, jnp.maximum(out, 0.0).astype(BF16))
        return carry

    lax.fori_loop(0, count // group, some, 0)


def layer_weights(refs, l):
    return jnp.concatenate([ref[l].astype(F32).T.astype(BF16) for ref in refs], axis=0)


def interact_kernel(place_ref, wq_ref, wk_ref, wv_ref, wr_ref, *refs, cuts, sources, group, part, opens):
    count = len(cuts) if opens else 1
    in_refs, o_ref = refs[:count], refs[count]
    refs = refs[count + 1 :]
    q_s, k_s, v_s, r_s, a_s = refs[-5:]
    chips, out_slots, width, lanes = o_ref.shape
    fields = q_s.shape[0]
    layers = wq_ref.shape[0]
    size = width // HEADS
    per = len(sources)
    whole = chips * per == fields
    weights = (wq_ref, wk_ref, wv_ref, wr_ref)

    if opens:
        x_s, h_s = refs[-6], refs[0]

        def gather(i, carry):
            for local, parts in enumerate(sources):
                found = None
                for r, j in parts:
                    cut = next(n for n, (low, high) in enumerate(cuts) if low <= j < high)
                    piece = in_refs[cut][i, r, j - cuts[cut][0]]
                    found = piece if found is None else found + piece
                x_s[i * per + local] = found
            return carry

        lax.fori_loop(0, chips, gather, 0)
    else:
        h_s = in_refs[0]

    for l in range(0 if opens else layers - 1, layers):
        if l == 0:
            load = lambda f: x_s[f if whole else place_ref[f]]
        else:
            load = lambda f: h_s[f]
        project(load, layer_weights(weights, l), q_s, k_s, v_s, r_s, fields, width, lanes)
        if l < layers - 1:

            def store(f, at, out):
                h_s[f, at : at + size, :] = out

            attend(q_s, k_s, v_s, r_s, a_s, store, lambda f: f, fields, fields, width, group)
        elif whole:

            def store(n, at, out):
                o_ref[lax.rem(n, chips), lax.div(n, chips), at : at + size, :] = out

            def field_of(n):
                return lax.rem(n, chips) * per + lax.div(n, chips) + part[0]

            total = chips * out_slots
            attend(q_s, k_s, v_s, r_s, a_s, store, field_of, total, fields, width, group)
        else:

            def clear(i, carry):
                for local in range(out_slots):
                    o_ref[i, local] = jnp.zeros((width, lanes), BF16)
                return carry

            lax.fori_loop(0, chips, clear, 0)

            def store(f, at, out):
                slot = place_ref[f]
                o_ref[lax.div(slot, per), lax.rem(slot, per), at : at + size, :] = out

            attend(q_s, k_s, v_s, r_s, a_s, store, lambda f: f, fields, fields, width, group)


def interact(place, given, chips, cuts, weights, sources, fields, part, opens, more):
    width, lanes = given[0].shape[-2:]
    group = divisor(fields, (4, 2, 1))
    wide = pltpu.VMEM((fields, width, lanes), F32)
    vmem = pl.BlockSpec(memory_space=pltpu.VMEM)
    layer_in = jax.ShapeDtypeStruct((fields, width, lanes), BF16)
    outs = [jax.ShapeDtypeStruct((chips, part[1] - part[0], width, lanes), BF16)]
    scratch = [
        wide,
        pltpu.VMEM((width * fields, lanes), F32),
        wide,
        wide,
        pltpu.VMEM((group * fields, lanes), F32),
    ]
    if opens:
        scratch = [pltpu.VMEM((chips * len(sources), width, lanes), BF16)] + scratch
        if more:
            outs.append(layer_in)
        else:
            scratch = [pltpu.VMEM((fields, width, lanes), BF16)] + scratch
    return pl.pallas_call(
        functools.partial(
            interact_kernel, cuts=tuple(cuts), sources=sources, group=group, part=part, opens=opens
        ),
        out_shape=outs,
        in_specs=[pl.BlockSpec(memory_space=pltpu.SMEM)] + [vmem] * (4 + len(given)),
        out_specs=[vmem] * len(outs),
        scratch_shapes=scratch,
        compiler_params=pltpu.CompilerParams(vmem_limit_bytes=VMEM_BYTES),
        cost_estimate=pl.CostEstimate(
            flops=12_000_000_000, bytes_accessed=4_000_000, transcendentals=0
        ),
    )(place, *weights, *given)


def per_device(
    feature_ids,
    field_slot,
    table,
    query_weight,
    key_weight,
    value_weight,
    residual_weight,
    out_weight,
):
    total, per = feature_ids.shape
    owned, width = table.shape
    chips = lax.axis_size("fld")
    reps = lax.axis_size("rep")
    half = total // reps
    peer = half // chips
    blocks = chips * reps
    rows_slot = owned * reps // per
    slot_count = chips * per
    fields = field_slot.shape[0]

    spans = [(r * owned // rows_slot, -(-(r + 1) * owned // rows_slot)) for r in range(reps)]
    held = max(b - a for a, b in spans)
    held_slots = [[min(a, per - held) + j for j in range(held)] for a, _ in spans]
    sources = tuple(
        tuple((r, held_slots[r].index(s)) for r in range(reps) if spans[r][0] <= s < spans[r][1])
        for s in range(per)
    )
    step = divisor(owned, (16384, 8192, 4096, 2048, 1024, 512, 256))
    slot_ids = jnp.transpose(feature_ids)
    table_t = jnp.transpose(table)
    ranks = range(reps)

    def look_up(low, high):
        shift_of = [
            [(held_slots[r][j]) * rows_slot - r * owned for r in ranks] for j in range(low, high)
        ]
        starts = [max(0, shift_of[0][r]) // step for r in ranks]
        bounds_of = [starts] + [
            [max(starts[r], min(owned // step, -(-(shift[r] + rows_slot) // step))) for r in ranks]
            for shift in shift_of
        ]
        most = max(end - start for end, start in zip(bounds_of[-1], starts)) * step
        slot_of = [[held_slots[r][j] for r in ranks] for j in range(low, high)]
        return lookup(slot_ids, table_t, blocks, slot_of, shift_of, bounds_of, step, most)

    def exchange(found):
        arrived = lax.all_to_all(found, ("fld", "rep"), 0, 0, tiled=True)
        return arrived.reshape(chips, reps, found.shape[1], width, peer)

    cuts = [(0, held)]
    founds = []
    for cut in cuts:
        founds.append(look_up(*cut))
    arrived = []
    for found in founds:
        arrived.append(exchange(found))
    weights = (query_weight, key_weight, value_weight, residual_weight)

    parts = parts_of(per)
    given = arrived
    hidden, sent = [], []
    for n, part in enumerate(parts):
        more = n + 1 < len(parts)
        done = interact(
            field_slot, given, chips, cuts, weights, sources, fields, part, n == 0, more
        )
        hidden.append(done[0])
        given = done[1:] if n == 0 else given
    for block in hidden:
        sent.append(lax.all_to_all(block, "fld", 0, 0, tiled=True))
    select = (field_slot[:, None] == jnp.arange(slot_count, dtype=jnp.int32)[None, :]).astype(F32)
    slot_weight = jnp.einsum("fs,fd->sd", select, out_weight, precision=lax.Precision.HIGHEST)
    slot_weight = slot_weight.reshape(chips, per, width)
    logits = sum(
        jnp.einsum(
            "csdn,csd->n",
            block.astype(F32),
            slot_weight[:, low:high],
            precision=lax.Precision.HIGHEST,
        )
        for block, (low, high) in zip(hidden, parts)
    )
    interacted = jnp.concatenate(
        [x.transpose(1, 0, 3, 2).reshape(x.shape[1], half, width) for x in sent], axis=0
    )
    return (interacted, logits.reshape(1, peer))


def parts_of(per):
    return [(0, per)]


def solution(mesh):
    placed = (P("groups", "fld"), P(), P(("fld", "rep"), None), P(), P(), P(), P(), P())

    return jax.shard_map(
        per_device,
        mesh=mesh,
        in_specs=placed,
        out_specs=(P("fld", ("groups", "rep"), None), P("rep", ("groups", "fld"))),
        check_vma=False,
    )
```

```python
import functools
import math

import jax
import jax.numpy as jnp
from jax import lax
from jax.experimental import pallas as pl
from jax.experimental.pallas import tpu as pltpu
from jax.sharding import PartitionSpec as P

HEADS = 2
F32 = jnp.float32
BF16 = jnp.bfloat16
LANES = 128
VMEM_BYTES = 58 * 1024 * 1024


def divisor(count, options):
    return next(c for c in options if count % c == 0)


def by_rep(options):
    rep = lax.axis_index("rep")
    found = jnp.int32(options[0])
    for r, option in enumerate(options[1:], 1):
        found = jnp.where(rep == r, jnp.int32(option), found)
    return found


def lookup_kernel(
    ids_ref, tab_ref, *refs, step, slot_of, shift_of, bounds_of, owned
):
    out_ref, land, tab, stage, lines, odd_ref, row_ref, sem, row_sem = refs[-9:]
    blocks, slots, width, lanes = out_ref.shape
    reps = len(bounds_of[0])
    rep = lax.axis_index("rep")
    buffers = land.shape[0]
    batch = stage.shape[0] // lanes
    spare = tab.shape[0] - 8
    bounds = [by_rep(b) for b in bounds_of]
    first, last = bounds[0], bounds[-1]
    pairs = step // (2 * lanes)

    def fetch(c):
        b = lax.rem(c, buffers)
        at = pl.ds(pl.multiple_of(c * step, step), step)
        return pltpu.make_async_copy(tab_ref.at[:, at], land.at[b], sem.at[b])

    for i in range(buffers):

        @pl.when(first + i < last)
        def _():
            fetch(first + i).start()

    tab[pl.ds(spare, 8), :] = jnp.zeros((8, 2 * width), F32)
    for j in range(slots):
        shift = by_rep(shift_of[j])
        for b in range(blocks):
            at = ((b % reps) * (blocks // reps) + b // reps) * lanes
            rows = ids_ref[slot_of[j][0] : slot_of[j][0] + 1, at : at + lanes]
            for r, slot in enumerate(slot_of[j][1:], 1):
                rows = jnp.where(rep == r, ids_ref[slot : slot + 1, at : at + lanes], rows)
            rows = rows + shift
            here = (rows >= 0) & (rows < owned)
            rows = rows - first * step
            line = ((rows >> 8) << 7) | (rows & (lanes - 1))
            lines[pl.ds(j * blocks + b, 1), :] = jnp.where(here, line, spare)
            odd_ref[pl.ds(j * blocks + b, 1), :] = (rows >> 7) & 1
    rows_copy = pltpu.make_async_copy(lines, row_ref, row_sem)
    rows_copy.start()
    rows_copy.wait()
    for j in range(slots):

        def chunk(c, carry):
            fetch(c).wait()
            b = lax.rem(c, buffers)

            def turn(p, carry):
                at = pl.multiple_of(p * (2 * lanes), 2 * lanes)
                two = jnp.concatenate(
                    [land[b, :, pl.ds(at, lanes)], land[b, :, pl.ds(at + lanes, lanes)]], axis=0
                )
                to = pl.multiple_of((c - first) * (step // 2) + p * lanes, lanes)
                tab[pl.ds(to, lanes), :] = two.T.astype(F32)
                return carry

            lax.fori_loop(0, pairs, turn, 0, unroll=min(pairs, 64))

            @pl.when(c + buffers < last)
            def _():
                fetch(c + buffers).start()

            return carry

        lax.fori_loop(bounds[j], bounds[j + 1], chunk, 0)

        def some_blocks(i, carry, j=j):
            def some(n, carry):
                at = j * blocks + i * batch + n
                to = n * lanes
                for u in range(lanes):
                    stage[pl.ds(to + u, 1), :] = tab[pl.ds(row_ref[at, u], 1), :]
                return carry

            lax.fori_loop(0, batch, some, 0)
            for g in range(batch):
                b = i * batch + g
                turned = stage[g * lanes : (g + 1) * lanes].astype(BF16).T.astype(F32)
                odd = odd_ref[pl.ds(j * blocks + b, 1), :] > 0
                out_ref[b, j] = jnp.where(odd, turned[width:], turned[:width]).astype(BF16)
            return carry

        lax.fori_loop(0, blocks // batch, some_blocks, 0)


def lookup(ids, table_t, blocks, slot_of, shift_of, bounds_of, step, most):
    width, owned = table_t.shape
    slots = len(slot_of)
    buffers = min(4, owned // step)
    batch = divisor(blocks, (4, 2, 1))
    vmem = pl.BlockSpec(memory_space=pltpu.VMEM)
    anywhere = pl.BlockSpec(memory_space=pl.ANY)
    return pl.pallas_call(
        functools.partial(
            lookup_kernel,
            step=step,
            slot_of=slot_of,
            shift_of=shift_of,
            bounds_of=bounds_of,
            owned=owned,
        ),
        out_shape=jax.ShapeDtypeStruct((blocks, slots, width, LANES), BF16),
        in_specs=[vmem, anywhere],
        out_specs=vmem,
        scratch_shapes=[
            pltpu.VMEM((buffers, width, step), BF16),
            pltpu.VMEM((most // 2 + 8, 2 * width), F32),
            pltpu.VMEM((batch * LANES, 2 * width), F32),
            pltpu.VMEM((slots * blocks, LANES), jnp.int32),
            pltpu.VMEM((slots * blocks, LANES), jnp.int32),
            pltpu.SMEM((slots * blocks, LANES), jnp.int32),
            pltpu.SemaphoreType.DMA((buffers,)),
            pltpu.SemaphoreType.DMA,
        ],
        compiler_params=pltpu.CompilerParams(vmem_limit_bytes=VMEM_BYTES),
        cost_estimate=pl.CostEstimate(
            flops=slots * 12_000_000_000, bytes_accessed=2 * most * width, transcendentals=0
        ),
    )(ids, table_t)


ROWS = 8
CHAINS = 4


def project(load, w, q_s, kt_s, k_s, v_s, r_s):
    fields, width, lanes = q_s.shape

    def pair(i, carry):
        f = 2 * i
        x2 = jnp.concatenate([load(f), load(f + 1)], axis=1)
        y = lax.dot_general(w, x2, (((1,), (0,)), ((), ())), preferred_element_type=F32)
        ys = [y[:, :lanes], y[:, lanes:]]
        for u in range(2):
            q_s[f + u] = ys[u][:width]
            kt_s[pl.ds(f + u, width, stride=fields), :] = ys[u][width : 2 * width]
            r_s[f + u] = ys[u][3 * width :]
        for t in range(width // ROWS):
            at = 2 * width + ROWS * t
            two = jnp.concatenate([yu[at : at + ROWS] for yu in ys], axis=0)
            v_s[i, 2 * ROWS * t : 2 * ROWS * (t + 1)] = two.astype(BF16)
        return carry

    lax.fori_loop(0, fields // 2, pair, 0, unroll=divisor(fields // 2, (10, 8, 5, 4, 2, 1)))

    def turn(i, carry):
        rows = [
            kt_s[pl.ds(pl.multiple_of((2 * i + u) * fields, ROWS), fields), :] for u in range(2)
        ]
        for t in range(fields // ROWS):
            two = jnp.concatenate([x[ROWS * t : ROWS * (t + 1)] for x in rows], axis=0)
            k_s[i, 2 * ROWS * t : 2 * ROWS * (t + 1)] = two.astype(BF16)
        return carry

    lax.fori_loop(0, width // 2, turn, 0, unroll=4)


def spread(a, b):
    shape = (ROWS, a.shape[1])
    two = jnp.concatenate([jnp.broadcast_to(a, shape), jnp.broadcast_to(b, shape)], axis=0)
    return two.astype(BF16).astype(F32)


def halves(x):
    return x[:ROWS] + x[ROWS:]


def attend(q_s, k_s, v_s, r_s, a_s, store, field_of, count, group):
    fields, width, _ = q_s.shape
    size = width // HEADS
    scale = math.log2(math.e) / math.sqrt(size)
    tiles = fields // ROWS
    whole = tiles // CHAINS * CHAINS
    jobs = [
        [(u, t) for t in range(n, n + CHAINS)] for n in range(0, whole, CHAINS) for u in range(group)
    ]
    left = [(u, t) for t in range(whole, tiles) for u in range(group)]
    jobs += [left[n : n + CHAINS] for n in range(0, len(left), CHAINS)]

    def some(i, carry):
        own = [field_of(i * group + u) for u in range(group)]
        for h in range(HEADS):
            scores = {}
            for job in jobs:
                sums = {}
                for d in range(h * size, (h + 1) * size, 2):
                    qs = {
                        u: spread(q_s[own[u], pl.ds(d, 1), :], q_s[own[u], pl.ds(d + 1, 1), :])
                        for u, _ in job
                    }
                    for u, t in job:
                        match = k_s[d // 2, 2 * ROWS * t : 2 * ROWS * (t + 1), :].astype(F32)
                        term = match * qs[u]
                        sums[u, t] = sums[u, t] + term if (u, t) in sums else term
                scores.update((key, halves(x)) for key, x in sums.items())
            for u in range(group):
                score = jnp.concatenate([scores[u, t] for t in range(tiles)], axis=0)
                top = jnp.max(score, axis=0, keepdims=True)
                e = jnp.exp2((score - top) * scale)
                a_s[u * fields : (u + 1) * fields, :] = e / jnp.sum(e, axis=0, keepdims=True)
            for u in range(group):
                sums = {}
                for g in range(0, fields, 2):
                    at = u * fields + g
                    weight = spread(a_s[at : at + 1, :], a_s[at + 1 : at + 2, :])
                    for t in range(h * size // ROWS, (h + 1) * size // ROWS):
                        content = v_s[g // 2, 2 * ROWS * t : 2 * ROWS * (t + 1), :].astype(F32)
                        term = content * weight
                        sums[t] = sums[t] + term if t in sums else term
                mixed = jnp.concatenate([halves(x) for x in sums.values()], axis=0)
                out = mixed + r_s[own[u], h * size : (h + 1) * size, :]
                store(i * group + u, h * size, jnp.maximum(out, 0.0).astype(BF16))
        return carry

    lax.fori_loop(0, count // group, some, 0)


def layer_weights(refs, l):
    return jnp.concatenate([ref[l].astype(F32).T.astype(BF16) for ref in refs], axis=0)


def interact_kernel(place_ref, wq_ref, wk_ref, wv_ref, wr_ref, *refs, cuts, sources, group, part, opens):
    count = len(cuts) if opens else 1
    in_refs, o_ref = refs[:count], refs[count]
    refs = refs[count + 1 :]
    q_s, kt_s, k_s, v_s, r_s, a_s = refs[-6:]
    chips, out_slots, width, lanes = o_ref.shape
    fields = q_s.shape[0]
    layers = wq_ref.shape[0]
    size = width // HEADS
    per = len(sources)
    whole = chips * per == fields
    weights = (wq_ref, wk_ref, wv_ref, wr_ref)

    if opens:
        x_s, h_s = refs[-7], refs[0]

        def gather(i, carry):
            for local, parts in enumerate(sources):
                found = None
                for r, j in parts:
                    cut = next(n for n, (low, high) in enumerate(cuts) if low <= j < high)
                    piece = in_refs[cut][i, r, j - cuts[cut][0]]
                    found = piece if found is None else found + piece
                x_s[i * per + local] = found
            return carry

        lax.fori_loop(0, chips, gather, 0)
    else:
        h_s = in_refs[0]

    for l in range(0 if opens else layers - 1, layers):
        if l == 0:
            load = lambda f: x_s[f if whole else place_ref[f]]
        else:
            load = lambda f: h_s[f]
        project(load, layer_weights(weights, l), q_s, kt_s, k_s, v_s, r_s)
        if l < layers - 1:

            def store(f, at, out):
                h_s[f, at : at + size, :] = out

            attend(q_s, k_s, v_s, r_s, a_s, store, lambda f: f, fields, group)
        elif whole:

            def store(n, at, out):
                o_ref[lax.rem(n, chips), lax.div(n, chips), at : at + size, :] = out

            def field_of(n):
                return lax.rem(n, chips) * per + lax.div(n, chips) + part[0]

            total = chips * out_slots
            attend(q_s, k_s, v_s, r_s, a_s, store, field_of, total, group)
        else:

            def clear(i, carry):
                for local in range(out_slots):
                    o_ref[i, local] = jnp.zeros((width, lanes), BF16)
                return carry

            lax.fori_loop(0, chips, clear, 0)

            def store(f, at, out):
                slot = place_ref[f]
                o_ref[lax.div(slot, per), lax.rem(slot, per), at : at + size, :] = out

            attend(q_s, k_s, v_s, r_s, a_s, store, lambda f: f, fields, group)


def interact(place, given, chips, cuts, weights, sources, fields, part, opens, more):
    width, lanes = given[0].shape[-2:]
    group = divisor(fields, (4, 2, 1))
    wide = pltpu.VMEM((fields, width, lanes), F32)
    vmem = pl.BlockSpec(memory_space=pltpu.VMEM)
    layer_in = jax.ShapeDtypeStruct((fields, width, lanes), BF16)
    outs = [jax.ShapeDtypeStruct((chips, part[1] - part[0], width, lanes), BF16)]
    scratch = [
        wide,
        pltpu.VMEM((width * fields, lanes), F32),
        pltpu.VMEM((width // 2, 2 * fields, lanes), BF16),
        pltpu.VMEM((fields // 2, 2 * width, lanes), BF16),
        wide,
        pltpu.VMEM((group * fields, lanes), F32),
    ]
    if opens:
        scratch = [pltpu.VMEM((chips * len(sources), width, lanes), BF16)] + scratch
        if more:
            outs.append(layer_in)
        else:
            scratch = [pltpu.VMEM((fields, width, lanes), BF16)] + scratch
    return pl.pallas_call(
        functools.partial(
            interact_kernel, cuts=tuple(cuts), sources=sources, group=group, part=part, opens=opens
        ),
        out_shape=outs,
        in_specs=[pl.BlockSpec(memory_space=pltpu.SMEM)] + [vmem] * (4 + len(given)),
        out_specs=[vmem] * len(outs),
        scratch_shapes=scratch,
        compiler_params=pltpu.CompilerParams(vmem_limit_bytes=VMEM_BYTES),
        cost_estimate=pl.CostEstimate(
            flops=12_000_000_000, bytes_accessed=4_000_000, transcendentals=0
        ),
    )(place, *weights, *given)


def per_device(
    feature_ids,
    field_slot,
    table,
    query_weight,
    key_weight,
    value_weight,
    residual_weight,
    out_weight,
):
    total, per = feature_ids.shape
    owned, width = table.shape
    chips = lax.axis_size("fld")
    reps = lax.axis_size("rep")
    half = total // reps
    peer = half // chips
    blocks = chips * reps
    rows_slot = owned * reps // per
    slot_count = chips * per
    fields = field_slot.shape[0]

    spans = [(r * owned // rows_slot, -(-(r + 1) * owned // rows_slot)) for r in range(reps)]
    held = max(b - a for a, b in spans)
    held_slots = [[min(a, per - held) + j for j in range(held)] for a, _ in spans]
    sources = tuple(
        tuple((r, held_slots[r].index(s)) for r in range(reps) if spans[r][0] <= s < spans[r][1])
        for s in range(per)
    )
    step = divisor(owned, (16384, 8192, 4096, 2048, 1024, 512, 256))
    slot_ids = jnp.transpose(feature_ids)
    table_t = jnp.transpose(table)
    ranks = range(reps)

    def look_up(low, high):
        shift_of = [
            [(held_slots[r][j]) * rows_slot - r * owned for r in ranks] for j in range(low, high)
        ]
        starts = [max(0, shift_of[0][r]) // step for r in ranks]
        bounds_of = [starts] + [
            [max(starts[r], min(owned // step, -(-(shift[r] + rows_slot) // step))) for r in ranks]
            for shift in shift_of
        ]
        most = max(end - start for end, start in zip(bounds_of[-1], starts)) * step
        slot_of = [[held_slots[r][j] for r in ranks] for j in range(low, high)]
        return lookup(slot_ids, table_t, blocks, slot_of, shift_of, bounds_of, step, most)

    def exchange(found):
        arrived = lax.all_to_all(found, ("fld", "rep"), 0, 0, tiled=True)
        return arrived.reshape(chips, reps, found.shape[1], width, peer)

    cuts = [(0, held)]
    founds = []
    for cut in cuts:
        founds.append(look_up(*cut))
    arrived = []
    for found in founds:
        arrived.append(exchange(found))
    weights = (query_weight, key_weight, value_weight, residual_weight)

    parts = parts_of(per)
    given = arrived
    hidden, sent = [], []
    for n, part in enumerate(parts):
        more = n + 1 < len(parts)
        done = interact(
            field_slot, given, chips, cuts, weights, sources, fields, part, n == 0, more
        )
        hidden.append(done[0])
        given = done[1:] if n == 0 else given
    for block in hidden:
        sent.append(lax.all_to_all(block, "fld", 0, 0, tiled=True))
    select = (field_slot[:, None] == jnp.arange(slot_count, dtype=jnp.int32)[None, :]).astype(F32)
    slot_weight = jnp.einsum("fs,fd->sd", select, out_weight, precision=lax.Precision.HIGHEST)
    slot_weight = slot_weight.reshape(chips, per, width)
    logits = sum(
        jnp.einsum(
            "csdn,csd->n",
            block.astype(F32),
            slot_weight[:, low:high],
            precision=lax.Precision.HIGHEST,
        )
        for block, (low, high) in zip(hidden, parts)
    )
    interacted = jnp.concatenate(
        [x.transpose(1, 0, 3, 2).reshape(x.shape[1], half, width) for x in sent], axis=0
    )
    return (interacted, logits.reshape(1, peer))


def parts_of(per):
    return [(0, per)]


def solution(mesh):
    placed = (P("groups", "fld"), P(), P(("fld", "rep"), None), P(), P(), P(), P(), P())

    return jax.shard_map(
        per_device,
        mesh=mesh,
        in_specs=placed,
        out_specs=(P("fld", ("groups", "rep"), None), P("rep", ("groups", "fld"))),
        check_vma=False,
    )
```

```python
import functools
import math

import jax
import jax.numpy as jnp
from jax import lax
from jax.experimental import pallas as pl
from jax.experimental.pallas import tpu as pltpu
from jax.sharding import PartitionSpec as P

HEADS = 2
F32 = jnp.float32
BF16 = jnp.bfloat16
LANES = 128
VMEM_BYTES = 58 * 1024 * 1024


def divisor(count, options):
    return next(c for c in options if count % c == 0)


def by_rep(options):
    rep = lax.axis_index("rep")
    found = jnp.int32(options[0])
    for r, option in enumerate(options[1:], 1):
        found = jnp.where(rep == r, jnp.int32(option), found)
    return found


def lookup_kernel(
    ids_ref, tab_ref, *refs, step, slot_of, shift_of, bounds_of, owned
):
    outs = refs[:-8]
    land, tab, stage, lines, odd_ref, row_ref, sem, row_sem = refs[-8:]
    chips, slots, width, lanes = outs[0].shape
    reps = len(bounds_of[0])
    blocks = chips * reps
    chip = lax.axis_index("fld")
    rep = lax.axis_index("rep")
    buffers = land.shape[0]
    batch = stage.shape[0] // lanes
    spare = tab.shape[0] - 8
    bounds = [by_rep(b) for b in bounds_of]
    first, last = bounds[0], bounds[-1]
    pairs = step // (2 * lanes)

    def fetch(c):
        b = lax.rem(c, buffers)
        at = pl.ds(pl.multiple_of(c * step, step), step)
        return pltpu.make_async_copy(tab_ref.at[:, at], land.at[b], sem.at[b])

    for i in range(buffers):

        @pl.when(first + i < last)
        def _():
            fetch(first + i).start()

    tab[pl.ds(spare, 8), :] = jnp.zeros((8, 2 * width), F32)
    for j in range(slots):
        shift = by_rep(shift_of[j])
        for b in range(blocks):
            to_rep = lax.rem(rep + b // chips, reps)
            to_chip = lax.rem(chip + b % chips, chips)
            at = pl.ds(pl.multiple_of((to_rep * chips + to_chip) * lanes, lanes), lanes)
            rows = ids_ref[slot_of[j][0] : slot_of[j][0] + 1, at]
            for r, slot in enumerate(slot_of[j][1:], 1):
                rows = jnp.where(rep == r, ids_ref[slot : slot + 1, at], rows)
            rows = rows + shift
            here = (rows >= 0) & (rows < owned)
            rows = rows - first * step
            line = ((rows >> 8) << 7) | (rows & (lanes - 1))
            lines[pl.ds(j * blocks + b, 1), :] = jnp.where(here, line, spare)
            odd_ref[pl.ds(j * blocks + b, 1), :] = (rows >> 7) & 1
    rows_copy = pltpu.make_async_copy(lines, row_ref, row_sem)
    rows_copy.start()
    rows_copy.wait()
    for j in range(slots):

        def chunk(c, carry):
            fetch(c).wait()
            b = lax.rem(c, buffers)

            def turn(p, carry):
                at = pl.multiple_of(p * (2 * lanes), 2 * lanes)
                two = jnp.concatenate(
                    [land[b, :, pl.ds(at, lanes)], land[b, :, pl.ds(at + lanes, lanes)]], axis=0
                )
                to = pl.multiple_of((c - first) * (step // 2) + p * lanes, lanes)
                tab[pl.ds(to, lanes), :] = two.T.astype(F32)
                return carry

            lax.fori_loop(0, pairs, turn, 0, unroll=min(pairs, 64))

            @pl.when(c + buffers < last)
            def _():
                fetch(c + buffers).start()

            return carry

        lax.fori_loop(bounds[j], bounds[j + 1], chunk, 0)

        def some_blocks(i, carry, j=j, out_ref=None, ahead=0):
            def some(n, carry):
                at = j * blocks + ahead + i * batch + n
                to = n * lanes
                for u in range(lanes):
                    stage[pl.ds(to + u, 1), :] = tab[pl.ds(row_ref[at, u], 1), :]
                return carry

            lax.fori_loop(0, batch, some, 0)
            for g in range(batch):
                b = i * batch + g
                turned = stage[g * lanes : (g + 1) * lanes].astype(BF16).T.astype(F32)
                odd = odd_ref[pl.ds(j * blocks + ahead + b, 1), :] > 0
                out_ref[b, j] = jnp.where(odd, turned[width:], turned[:width]).astype(BF16)
            return carry

        for n, out_ref in enumerate(outs):
            here = functools.partial(some_blocks, out_ref=out_ref, ahead=n * chips)
            lax.fori_loop(0, chips // batch, here, 0)


def lookup(ids, table_t, chips, slot_of, shift_of, bounds_of, step, most):
    width, owned = table_t.shape
    slots = len(slot_of)
    buffers = min(4, owned // step)
    reps = len(bounds_of[0])
    blocks = chips * reps
    batch = divisor(chips, (4, 2, 1))
    vmem = pl.BlockSpec(memory_space=pltpu.VMEM)
    anywhere = pl.BlockSpec(memory_space=pl.ANY)
    return pl.pallas_call(
        functools.partial(
            lookup_kernel,
            step=step,
            slot_of=slot_of,
            shift_of=shift_of,
            bounds_of=bounds_of,
            owned=owned,
        ),
        out_shape=[jax.ShapeDtypeStruct((chips, slots, width, LANES), BF16)] * reps,
        in_specs=[vmem, anywhere],
        out_specs=[vmem] * reps,
        scratch_shapes=[
            pltpu.VMEM((buffers, width, step), BF16),
            pltpu.VMEM((most // 2 + 8, 2 * width), F32),
            pltpu.VMEM((batch * LANES, 2 * width), F32),
            pltpu.VMEM((slots * blocks, LANES), jnp.int32),
            pltpu.VMEM((slots * blocks, LANES), jnp.int32),
            pltpu.SMEM((slots * blocks, LANES), jnp.int32),
            pltpu.SemaphoreType.DMA((buffers,)),
            pltpu.SemaphoreType.DMA,
        ],
        compiler_params=pltpu.CompilerParams(vmem_limit_bytes=VMEM_BYTES),
        cost_estimate=pl.CostEstimate(
            flops=slots * 12_000_000_000, bytes_accessed=2 * most * width, transcendentals=0
        ),
    )(ids, table_t)


def pack_kernel(*refs, sources, reps, chips):
    found, outs = refs[:reps], refs[reps:]
    rep = lax.axis_index("rep")
    chip = lax.axis_index("fld")
    for k in range(chips):
        for s, parts in enumerate(sources):
            total = None
            for r, j in parts:
                piece = found[0][k, j]
                for n in range(1, reps):
                    piece = jnp.where(lax.rem(rep + reps - n, reps) == r, found[n][k, j], piece)
                total = piece if total is None else total + piece
            if len(outs) == chips:
                outs[k][s] = total
            else:
                outs[0][lax.rem(chip + k, chips), s] = total


def pack(found, sources, single):
    reps = len(found)
    chips, _, width, lanes = found[0].shape
    per = len(sources)
    vmem = pl.BlockSpec(memory_space=pltpu.VMEM)
    block = jax.ShapeDtypeStruct((per, width, lanes), BF16)
    outs = [jax.ShapeDtypeStruct((chips, *block.shape), BF16)] if single else [block] * chips
    return pl.pallas_call(
        functools.partial(pack_kernel, sources=sources, reps=reps, chips=chips),
        out_shape=outs,
        in_specs=[vmem] * reps,
        out_specs=[vmem] * len(outs),
        compiler_params=pltpu.CompilerParams(vmem_limit_bytes=VMEM_BYTES),
        name="pack",
    )(*found)


def join_kernel(*refs):
    parts, out_ref = refs[:-1], refs[-1]
    chips = len(parts)
    lanes = parts[0].shape[-1]
    chip = lax.axis_index("fld")
    for k, part in enumerate(parts):
        at = pl.multiple_of(lax.rem(chip + chips - k, chips) * lanes, lanes)
        out_ref[:, :, pl.ds(at, lanes)] = part[...]


def join(parts):
    per, width, lanes = parts[0].shape
    vmem = pl.BlockSpec(memory_space=pltpu.VMEM)
    return pl.pallas_call(
        join_kernel,
        out_shape=jax.ShapeDtypeStruct((per, width, lanes * len(parts)), BF16),
        in_specs=[vmem] * len(parts),
        out_specs=vmem,
        compiler_params=pltpu.CompilerParams(vmem_limit_bytes=VMEM_BYTES),
        name="join",
    )(*parts)


def swap(blocks):
    chips = len(blocks)
    out = [blocks[0]]
    for k in range(1, chips):
        out.append(lax.ppermute(blocks[k], "fld", [(i, (i + k) % chips) for i in range(chips)]))
    return out


ROWS = 8
CHAINS = 4


def project(load, w, q_s, kt_s, k_s, v_s, r_s):
    fields, width, lanes = q_s.shape

    def pair(i, carry):
        f = 2 * i
        x2 = jnp.concatenate([load(f), load(f + 1)], axis=1)
        y = lax.dot_general(w, x2, (((1,), (0,)), ((), ())), preferred_element_type=F32)
        ys = [y[:, :lanes], y[:, lanes:]]
        for u in range(2):
            q_s[f + u] = ys[u][:width]
            kt_s[pl.ds(f + u, width, stride=fields), :] = ys[u][width : 2 * width]
            r_s[f + u] = ys[u][3 * width :]
        for t in range(width // ROWS):
            at = 2 * width + ROWS * t
            two = jnp.concatenate([yu[at : at + ROWS] for yu in ys], axis=0)
            v_s[i, 2 * ROWS * t : 2 * ROWS * (t + 1)] = two.astype(BF16)
        return carry

    lax.fori_loop(0, fields // 2, pair, 0, unroll=divisor(fields // 2, (10, 8, 5, 4, 2, 1)))

    def turn(i, carry):
        rows = [
            kt_s[pl.ds(pl.multiple_of((2 * i + u) * fields, ROWS), fields), :] for u in range(2)
        ]
        for t in range(fields // ROWS):
            two = jnp.concatenate([x[ROWS * t : ROWS * (t + 1)] for x in rows], axis=0)
            k_s[i, 2 * ROWS * t : 2 * ROWS * (t + 1)] = two.astype(BF16)
        return carry

    lax.fori_loop(0, width // 2, turn, 0, unroll=4)


def spread(a, b):
    shape = (ROWS, a.shape[1])
    two = jnp.concatenate([jnp.broadcast_to(a, shape), jnp.broadcast_to(b, shape)], axis=0)
    return two.astype(BF16).astype(F32)


def halves(x):
    return x[:ROWS] + x[ROWS:]


def attend(q_s, k_s, v_s, r_s, a_s, store, field_of, count, group):
    fields, width, _ = q_s.shape
    size = width // HEADS
    scale = math.log2(math.e) / math.sqrt(size)
    tiles = fields // ROWS
    whole = tiles // CHAINS * CHAINS
    jobs = [
        [(u, t) for t in range(n, n + CHAINS)] for n in range(0, whole, CHAINS) for u in range(group)
    ]
    left = [(u, t) for t in range(whole, tiles) for u in range(group)]
    jobs += [left[n : n + CHAINS] for n in range(0, len(left), CHAINS)]

    def some(i, carry):
        own = [field_of(i, u) for u in range(group)]
        for h in range(HEADS):
            scores = {}
            for job in jobs:
                sums = {}
                for d in range(h * size, (h + 1) * size, 2):
                    qs = {
                        u: spread(q_s[own[u], pl.ds(d, 1), :], q_s[own[u], pl.ds(d + 1, 1), :])
                        for u, _ in job
                    }
                    for u, t in job:
                        match = k_s[d // 2, 2 * ROWS * t : 2 * ROWS * (t + 1), :].astype(F32)
                        term = match * qs[u]
                        sums[u, t] = sums[u, t] + term if (u, t) in sums else term
                scores.update((key, halves(x)) for key, x in sums.items())
            for u in range(group):
                score = jnp.concatenate([scores[u, t] for t in range(tiles)], axis=0)
                top = jnp.max(score, axis=0, keepdims=True)
                e = jnp.exp2((score - top) * scale)
                a_s[u * fields : (u + 1) * fields, :] = e / jnp.sum(e, axis=0, keepdims=True)
            for u in range(group):
                sums = {}
                for g in range(0, fields, 2):
                    at = u * fields + g
                    weight = spread(a_s[at : at + 1, :], a_s[at + 1 : at + 2, :])
                    for t in range(h * size // ROWS, (h + 1) * size // ROWS):
                        content = v_s[g // 2, 2 * ROWS * t : 2 * ROWS * (t + 1), :].astype(F32)
                        term = content * weight
                        sums[t] = sums[t] + term if t in sums else term
                mixed = jnp.concatenate([halves(x) for x in sums.values()], axis=0)
                out = mixed + r_s[own[u], h * size : (h + 1) * size, :]
                store(i, u, h * size, jnp.maximum(out, 0.0).astype(BF16))
        return carry

    lax.fori_loop(0, count // group, some, 0)


def layer_weights(refs, l):
    return jnp.concatenate([ref[l].astype(F32).T.astype(BF16) for ref in refs], axis=0)


def interact_kernel(place_ref, wq_ref, wk_ref, wv_ref, wr_ref, *refs, chips, group, fields):
    q_s, kt_s, k_s, v_s, r_s, a_s, x_s, h_s = refs[-8:]
    blocks = (len(refs) - 8) // 2
    ins, outs = refs[:blocks], refs[blocks : 2 * blocks]
    per, width, lanes = ins[0].shape[-3:]
    layers = wq_ref.shape[0]
    size = width // HEADS
    whole = chips * per == fields
    chip = lax.axis_index("fld")
    weights = (wq_ref, wk_ref, wv_ref, wr_ref)

    def in_order(i, u):
        return i * group + u

    for k in range(chips):
        back = lax.rem(chip + chips - k, chips)
        for s in range(per):
            x_s[back * per + s] = ins[k][s] if blocks == chips else ins[0][back, s]

    for l in range(layers):
        if l == 0:
            load = lambda f: x_s[f if whole else place_ref[f]]
        else:
            load = lambda f: h_s[f]
        project(load, layer_weights(weights, l), q_s, kt_s, k_s, v_s, r_s)
        if l < layers - 1:

            def store(i, u, at, out):
                h_s[i * group + u, at : at + size, :] = out

            attend(q_s, k_s, v_s, r_s, a_s, store, in_order, fields, group)
        elif blocks == chips:
            for low in range(0, chips, group):

                def field_of(i, u, low=low):
                    return lax.rem(chip + low + u, chips) * per + i

                def store(i, u, at, out, low=low):
                    outs[low + u][i, at : at + size, :] = out

                attend(q_s, k_s, v_s, r_s, a_s, store, field_of, per * group, group)
        else:
            for k in range(chips if not whole else 0):
                for s in range(per):
                    outs[0][k, s] = jnp.zeros((width, lanes), BF16)

            def store(i, u, at, out):
                f = i * group + u
                slot = f if whole else place_ref[f]
                outs[0][lax.div(slot, per), lax.rem(slot, per), at : at + size, :] = out

            attend(q_s, k_s, v_s, r_s, a_s, store, in_order, fields, group)


def interact(place, given, chips, weights, fields):
    per, width, lanes = given[0].shape[-3:]
    group = divisor(math.gcd(fields, chips), (4, 2, 1))
    wide = pltpu.VMEM((fields, width, lanes), F32)
    vmem = pl.BlockSpec(memory_space=pltpu.VMEM)
    scratch = [
        wide,
        pltpu.VMEM((width * fields, lanes), F32),
        pltpu.VMEM((width // 2, 2 * fields, lanes), BF16),
        pltpu.VMEM((fields // 2, 2 * width, lanes), BF16),
        wide,
        pltpu.VMEM((group * fields, lanes), F32),
        pltpu.VMEM((chips * per, width, lanes), BF16),
        pltpu.VMEM((fields, width, lanes), BF16),
    ]
    return pl.pallas_call(
        functools.partial(interact_kernel, chips=chips, group=group, fields=fields),
        out_shape=[jax.ShapeDtypeStruct(x.shape, BF16) for x in given],
        in_specs=[pl.BlockSpec(memory_space=pltpu.SMEM)] + [vmem] * (4 + len(given)),
        out_specs=[vmem] * len(given),
        scratch_shapes=scratch,
        compiler_params=pltpu.CompilerParams(vmem_limit_bytes=VMEM_BYTES),
        cost_estimate=pl.CostEstimate(
            flops=12_000_000_000, bytes_accessed=4_000_000, transcendentals=0
        ),
        name="interact",
    )(place, *weights, *given)


def logit_kernel(w_ref, *refs):
    blocks, o_ref = refs[:-1], refs[-1]
    per, width, lanes = blocks[0].shape
    total = jnp.zeros((ROWS, lanes), F32)
    for k, block in enumerate(blocks):
        rest = w_ref[k : k + 1, :]
        pieces = []
        for _ in range(3):
            piece = rest.astype(BF16)
            rest = rest - piece.astype(F32)
            pieces.append(piece.astype(F32))
        pieces.append(jnp.zeros((ROWS - 3, per * width), F32))
        left = jnp.concatenate(pieces, axis=0).astype(BF16)
        right = block[...].reshape(per * width, lanes)
        total = total + jnp.dot(left, right, preferred_element_type=F32)
    o_ref[...] = jnp.sum(total, axis=0, keepdims=True)


def logit(weight, blocks):
    lanes = blocks[0].shape[-1]
    vmem = pl.BlockSpec(memory_space=pltpu.VMEM)
    return pl.pallas_call(
        logit_kernel,
        out_shape=jax.ShapeDtypeStruct((1, lanes), F32),
        in_specs=[vmem] * (1 + len(blocks)),
        out_specs=vmem,
        compiler_params=pltpu.CompilerParams(vmem_limit_bytes=VMEM_BYTES),
        cost_estimate=pl.CostEstimate(
            flops=1_000_000_000, bytes_accessed=1_000_000, transcendentals=0
        ),
        name="logit",
    )(weight, *blocks)


def per_device(
    feature_ids,
    field_slot,
    table,
    query_weight,
    key_weight,
    value_weight,
    residual_weight,
    out_weight,
):
    total, per = feature_ids.shape
    owned, width = table.shape
    chips = lax.axis_size("fld")
    reps = lax.axis_size("rep")
    half = total // reps
    peer = half // chips
    rows_slot = owned * reps // per
    slot_count = chips * per
    fields = field_slot.shape[0]

    spans = [(r * owned // rows_slot, -(-(r + 1) * owned // rows_slot)) for r in range(reps)]
    held = max(b - a for a, b in spans)
    held_slots = [[min(a, per - held) + j for j in range(held)] for a, _ in spans]
    sources = tuple(
        tuple((r, held_slots[r].index(s)) for r in range(reps) if spans[r][0] <= s < spans[r][1])
        for s in range(per)
    )
    step = divisor(owned, (16384, 8192, 4096, 2048, 1024, 512, 256))
    slot_ids = jnp.transpose(feature_ids)
    table_t = jnp.transpose(table)
    ranks = range(reps)

    def look_up(low, high):
        shift_of = [
            [(held_slots[r][j]) * rows_slot - r * owned for r in ranks] for j in range(low, high)
        ]
        starts = [max(0, shift_of[0][r]) // step for r in ranks]
        bounds_of = [starts] + [
            [max(starts[r], min(owned // step, -(-(shift[r] + rows_slot) // step))) for r in ranks]
            for shift in shift_of
        ]
        most = max(end - start for end, start in zip(bounds_of[-1], starts)) * step
        slot_of = [[held_slots[r][j] for r in ranks] for j in range(low, high)]
        return lookup(slot_ids, table_t, chips, slot_of, shift_of, bounds_of, step, most)

    found = look_up(0, held)
    found = [found[0]] + [
        lax.ppermute(found[n], "rep", [(r, (r + n) % reps) for r in ranks]) for n in range(1, reps)
    ]
    single = slot_count != fields or chips > 8
    blocks = pack(found, sources, single)

    def exchange(blocks):
        if single:
            return [lax.all_to_all(blocks[0], "fld", 0, 0, tiled=True)]
        return swap(blocks)

    weights = (query_weight, key_weight, value_weight, residual_weight)
    hidden = interact(field_slot, exchange(blocks), chips, weights, fields)
    sent = exchange(hidden)

    slots = jnp.arange(slot_count, dtype=jnp.int32)
    if not single:
        slots = (slots + lax.axis_index("fld") * per) % slot_count
    select = (field_slot[:, None] == slots[None, :]).astype(F32)
    slot_weight = jnp.einsum("fs,fd->sd", select, out_weight, precision=lax.Precision.HIGHEST)
    if single:
        logits = jnp.einsum(
            "csdn,csd->n",
            hidden[0].astype(F32),
            slot_weight.reshape(chips, per, width),
            precision=lax.Precision.HIGHEST,
        ).reshape(1, peer)
        joined = sent[0].transpose(1, 2, 0, 3).reshape(per, width, half)
    else:
        logits = logit(slot_weight.reshape(chips, per * width), hidden)
        joined = join(sent)
    return (jnp.transpose(joined, (0, 2, 1)), logits)


def solution(mesh):
    placed = (P("groups", "fld"), P(), P(("fld", "rep"), None), P(), P(), P(), P(), P())

    return jax.shard_map(
        per_device,
        mesh=mesh,
        in_specs=placed,
        out_specs=(P("fld", ("groups", "rep"), None), P("rep", ("groups", "fld"))),
        check_vma=False,
    )
```

```python
import functools
import math

import jax
import jax.numpy as jnp
from jax import lax
from jax.experimental import pallas as pl
from jax.experimental.pallas import tpu as pltpu
from jax.sharding import PartitionSpec as P

HEADS = 2
F32 = jnp.float32
BF16 = jnp.bfloat16
LANES = 128
VMEM_BYTES = 52 * 1024 * 1024
INTERACT_BYTES = 24 * 1024 * 1024
SMALL_BYTES = 8 * 1024 * 1024


def divisor(count, options):
    return next(c for c in options if count % c == 0)


def by_rep(options):
    rep = lax.axis_index("rep")
    found = jnp.int32(options[0])
    for r, option in enumerate(options[1:], 1):
        found = jnp.where(rep == r, jnp.int32(option), found)
    return found


def lookup_kernel(
    ids_ref, tab_ref, *refs, step, slot_of, shift_of, bounds_of, owned
):
    outs = refs[:-8]
    land, tab, stage, lines, odd_ref, row_ref, sem, row_sem = refs[-8:]
    chips, slots, width, lanes = outs[0].shape
    reps = len(bounds_of[0])
    blocks = chips * reps
    chip = lax.axis_index("fld")
    rep = lax.axis_index("rep")
    buffers = land.shape[0]
    batch = stage.shape[0] // lanes
    spare = tab.shape[0] - 8
    bounds = [by_rep(b) for b in bounds_of]
    first, last = bounds[0], bounds[-1]
    pairs = step // (2 * lanes)

    def fetch(c):
        b = lax.rem(c, buffers)
        at = pl.ds(pl.multiple_of(c * step, step), step)
        return pltpu.make_async_copy(tab_ref.at[:, at], land.at[b], sem.at[b])

    for i in range(buffers):

        @pl.when(first + i < last)
        def _():
            fetch(first + i).start()

    tab[pl.ds(spare, 8), :] = jnp.zeros((8, 2 * width), F32)
    for j in range(slots):
        shift = by_rep(shift_of[j])
        for b in range(blocks):
            to_rep = lax.rem(rep + b // chips, reps)
            to_chip = lax.rem(chip + b % chips, chips)
            at = pl.ds(pl.multiple_of((to_rep * chips + to_chip) * lanes, lanes), lanes)
            rows = ids_ref[slot_of[j][0] : slot_of[j][0] + 1, at]
            for r, slot in enumerate(slot_of[j][1:], 1):
                rows = jnp.where(rep == r, ids_ref[slot : slot + 1, at], rows)
            rows = rows + shift
            here = (rows >= 0) & (rows < owned)
            rows = rows - first * step
            line = ((rows >> 8) << 7) | (rows & (lanes - 1))
            lines[pl.ds(j * blocks + b, 1), :] = jnp.where(here, line, spare)
            odd_ref[pl.ds(j * blocks + b, 1), :] = (rows >> 7) & 1
    rows_copy = pltpu.make_async_copy(lines, row_ref, row_sem)
    rows_copy.start()
    rows_copy.wait()
    for j in range(slots):

        def chunk(c, carry):
            fetch(c).wait()
            b = lax.rem(c, buffers)

            def turn(p, carry):
                at = pl.multiple_of(p * (2 * lanes), 2 * lanes)
                two = jnp.concatenate(
                    [land[b, :, pl.ds(at, lanes)], land[b, :, pl.ds(at + lanes, lanes)]], axis=0
                )
                to = pl.multiple_of((c - first) * (step // 2) + p * lanes, lanes)
                tab[pl.ds(to, lanes), :] = two.T.astype(F32)
                return carry

            lax.fori_loop(0, pairs, turn, 0, unroll=min(pairs, 64))

            @pl.when(c + buffers < last)
            def _():
                fetch(c + buffers).start()

            return carry

        lax.fori_loop(bounds[j], bounds[j + 1], chunk, 0)

        def some_blocks(i, carry, j=j, out_ref=None, ahead=0):
            def some(n, carry):
                at = j * blocks + ahead + i * batch + n
                to = n * lanes
                for u in range(lanes):
                    stage[pl.ds(to + u, 1), :] = tab[pl.ds(row_ref[at, u], 1), :]
                return carry

            lax.fori_loop(0, batch, some, 0)
            for g in range(batch):
                b = i * batch + g
                turned = stage[g * lanes : (g + 1) * lanes].astype(BF16).T.astype(F32)
                odd = odd_ref[pl.ds(j * blocks + ahead + b, 1), :] > 0
                out_ref[b, j] = jnp.where(odd, turned[width:], turned[:width]).astype(BF16)
            return carry

        for n, out_ref in enumerate(outs):
            here = functools.partial(some_blocks, out_ref=out_ref, ahead=n * chips)
            lax.fori_loop(0, chips // batch, here, 0)


def lookup(ids, table_t, chips, slot_of, shift_of, bounds_of, step, most):
    width, owned = table_t.shape
    slots = len(slot_of)
    buffers = min(4, owned // step)
    reps = len(bounds_of[0])
    blocks = chips * reps
    batch = divisor(chips, (4, 2, 1))
    vmem = pl.BlockSpec(memory_space=pltpu.VMEM)
    anywhere = pl.BlockSpec(memory_space=pl.ANY)
    return pl.pallas_call(
        functools.partial(
            lookup_kernel,
            step=step,
            slot_of=slot_of,
            shift_of=shift_of,
            bounds_of=bounds_of,
            owned=owned,
        ),
        out_shape=[jax.ShapeDtypeStruct((chips, slots, width, LANES), BF16)] * reps,
        in_specs=[vmem, anywhere],
        out_specs=[vmem] * reps,
        scratch_shapes=[
            pltpu.VMEM((buffers, width, step), BF16),
            pltpu.VMEM((most // 2 + 8, 2 * width), F32),
            pltpu.VMEM((batch * LANES, 2 * width), F32),
            pltpu.VMEM((slots * blocks, LANES), jnp.int32),
            pltpu.VMEM((slots * blocks, LANES), jnp.int32),
            pltpu.SMEM((slots * blocks, LANES), jnp.int32),
            pltpu.SemaphoreType.DMA((buffers,)),
            pltpu.SemaphoreType.DMA,
        ],
        compiler_params=pltpu.CompilerParams(vmem_limit_bytes=VMEM_BYTES),
        cost_estimate=pl.CostEstimate(
            flops=slots * 12_000_000_000, bytes_accessed=2 * most * width, transcendentals=0
        ),
    )(ids, table_t)


def pack_kernel(*refs, sources, reps, chips):
    found, outs = refs[:reps], refs[reps:]
    rep = lax.axis_index("rep")
    chip = lax.axis_index("fld")
    for k in range(chips):
        for s, parts in enumerate(sources):
            total = None
            for r, j in parts:
                piece = found[0][k, j]
                for n in range(1, reps):
                    piece = jnp.where(lax.rem(rep + reps - n, reps) == r, found[n][k, j], piece)
                total = piece if total is None else total + piece
            if len(outs) == chips:
                outs[k][s] = total
            else:
                outs[0][lax.rem(chip + k, chips), s] = total


def pack(found, sources, single):
    reps = len(found)
    chips, _, width, lanes = found[0].shape
    per = len(sources)
    vmem = pl.BlockSpec(memory_space=pltpu.VMEM)
    block = jax.ShapeDtypeStruct((per, width, lanes), BF16)
    outs = [jax.ShapeDtypeStruct((chips, *block.shape), BF16)] if single else [block] * chips
    return pl.pallas_call(
        functools.partial(pack_kernel, sources=sources, reps=reps, chips=chips),
        out_shape=outs,
        in_specs=[vmem] * reps,
        out_specs=[vmem] * len(outs),
        compiler_params=pltpu.CompilerParams(vmem_limit_bytes=SMALL_BYTES),
        name="pack",
    )(*found)


def join_kernel(*refs):
    parts, out_ref, sem = refs[:-2], refs[-2], refs[-1]
    chips = len(parts)
    lanes = parts[0].shape[-1]
    chip = lax.axis_index("fld")
    copies = []
    for k, part in enumerate(parts):
        at = pl.multiple_of(lax.rem(chip + chips - k, chips) * lanes, lanes)
        copies.append(pltpu.make_async_copy(part, out_ref.at[:, :, pl.ds(at, lanes)], sem.at[k]))
    for copy in copies:
        copy.start()
    for copy in copies:
        copy.wait()


def join(parts):
    per, width, lanes = parts[0].shape
    anywhere = pl.BlockSpec(memory_space=pl.ANY)
    return pl.pallas_call(
        join_kernel,
        out_shape=jax.ShapeDtypeStruct((per, width, lanes * len(parts)), BF16),
        in_specs=[anywhere] * len(parts),
        out_specs=anywhere,
        scratch_shapes=[pltpu.SemaphoreType.DMA((len(parts),))],
        compiler_params=pltpu.CompilerParams(vmem_limit_bytes=SMALL_BYTES),
        name="join",
    )(*parts)


def swap(blocks):
    chips = len(blocks)
    out = [blocks[0]]
    for k in range(1, chips):
        out.append(lax.ppermute(blocks[k], "fld", [(i, (i + k) % chips) for i in range(chips)]))
    return out


ROWS = 8
CHAINS = 4


def project(load, w, q_s, kt_s, k_s, v_s, r_s):
    fields, width, lanes = q_s.shape

    def pair(i, carry):
        f = 2 * i
        x2 = jnp.concatenate([load(f), load(f + 1)], axis=1)
        y = lax.dot_general(w, x2, (((1,), (0,)), ((), ())), preferred_element_type=F32)
        ys = [y[:, :lanes], y[:, lanes:]]
        for u in range(2):
            q_s[f + u] = ys[u][:width]
            kt_s[pl.ds(f + u, width, stride=fields), :] = ys[u][width : 2 * width]
            r_s[f + u] = ys[u][3 * width :]
        for t in range(width // ROWS):
            at = 2 * width + ROWS * t
            two = jnp.concatenate([yu[at : at + ROWS] for yu in ys], axis=0)
            v_s[i, 2 * ROWS * t : 2 * ROWS * (t + 1)] = two.astype(BF16)
        return carry

    lax.fori_loop(0, fields // 2, pair, 0, unroll=divisor(fields // 2, (10, 8, 5, 4, 2, 1)))

    def turn(i, carry):
        rows = [
            kt_s[pl.ds(pl.multiple_of((2 * i + u) * fields, ROWS), fields), :] for u in range(2)
        ]
        for t in range(fields // ROWS):
            two = jnp.concatenate([x[ROWS * t : ROWS * (t + 1)] for x in rows], axis=0)
            k_s[i, 2 * ROWS * t : 2 * ROWS * (t + 1)] = two.astype(BF16)
        return carry

    lax.fori_loop(0, width // 2, turn, 0, unroll=4)


def spread(a, b):
    shape = (ROWS, a.shape[1])
    two = jnp.concatenate([jnp.broadcast_to(a, shape), jnp.broadcast_to(b, shape)], axis=0)
    return two.astype(BF16).astype(F32)


def halves(x):
    return x[:ROWS] + x[ROWS:]


def attend(q_s, k_s, v_s, r_s, a_s, store, field_of, count, group):
    fields, width, _ = q_s.shape
    size = width // HEADS
    scale = math.log2(math.e) / math.sqrt(size)
    tiles = fields // ROWS
    whole = tiles // CHAINS * CHAINS
    jobs = [
        [(u, t) for t in range(n, n + CHAINS)] for n in range(0, whole, CHAINS) for u in range(group)
    ]
    left = [(u, t) for t in range(whole, tiles) for u in range(group)]
    jobs += [left[n : n + CHAINS] for n in range(0, len(left), CHAINS)]

    def some(i, carry):
        own = [field_of(i, u) for u in range(group)]
        for h in range(HEADS):
            scores = {}
            for job in jobs:
                sums = {}
                for d in range(h * size, (h + 1) * size, 2):
                    qs = {
                        u: spread(q_s[own[u], pl.ds(d, 1), :], q_s[own[u], pl.ds(d + 1, 1), :])
                        for u, _ in job
                    }
                    for u, t in job:
                        match = k_s[d // 2, 2 * ROWS * t : 2 * ROWS * (t + 1), :].astype(F32)
                        term = match * qs[u]
                        sums[u, t] = sums[u, t] + term if (u, t) in sums else term
                scores.update((key, halves(x)) for key, x in sums.items())
            for u in range(group):
                score = jnp.concatenate([scores[u, t] for t in range(tiles)], axis=0)
                top = jnp.max(score, axis=0, keepdims=True)
                e = jnp.exp2((score - top) * scale)
                a_s[u * fields : (u + 1) * fields, :] = e / jnp.sum(e, axis=0, keepdims=True)
            for u in range(group):
                sums = {}
                for g in range(0, fields, 2):
                    at = u * fields + g
                    weight = spread(a_s[at : at + 1, :], a_s[at + 1 : at + 2, :])
                    for t in range(h * size // ROWS, (h + 1) * size // ROWS):
                        content = v_s[g // 2, 2 * ROWS * t : 2 * ROWS * (t + 1), :].astype(F32)
                        term = content * weight
                        sums[t] = sums[t] + term if t in sums else term
                mixed = jnp.concatenate([halves(x) for x in sums.values()], axis=0)
                out = mixed + r_s[own[u], h * size : (h + 1) * size, :]
                store(i, u, h * size, jnp.maximum(out, 0.0).astype(BF16))
        return carry

    lax.fori_loop(0, count // group, some, 0)


def layer_weights(refs, l):
    return jnp.concatenate([ref[l].astype(F32).T.astype(BF16) for ref in refs], axis=0)


def interact_kernel(place_ref, wq_ref, wk_ref, wv_ref, wr_ref, *refs, chips, group, fields):
    q_s, kt_s, k_s, v_s, r_s, a_s, x_s, h_s = refs[-8:]
    blocks = (len(refs) - 8) // 2
    ins, outs = refs[:blocks], refs[blocks : 2 * blocks]
    per, width, lanes = ins[0].shape[-3:]
    layers = wq_ref.shape[0]
    size = width // HEADS
    whole = chips * per == fields
    chip = lax.axis_index("fld")
    weights = (wq_ref, wk_ref, wv_ref, wr_ref)

    def in_order(i, u):
        return i * group + u

    for k in range(chips):
        back = lax.rem(chip + chips - k, chips)
        for s in range(per):
            x_s[back * per + s] = ins[k][s] if blocks == chips else ins[0][back, s]

    for l in range(layers):
        if l == 0:
            load = lambda f: x_s[f if whole else place_ref[f]]
        else:
            load = lambda f: h_s[f]
        project(load, layer_weights(weights, l), q_s, kt_s, k_s, v_s, r_s)
        if l < layers - 1:

            def store(i, u, at, out):
                h_s[i * group + u, at : at + size, :] = out

            attend(q_s, k_s, v_s, r_s, a_s, store, in_order, fields, group)
        elif blocks == chips:
            for low in range(0, chips, group):

                def field_of(i, u, low=low):
                    return lax.rem(chip + low + u, chips) * per + i

                def store(i, u, at, out, low=low):
                    outs[low + u][i, at : at + size, :] = out

                attend(q_s, k_s, v_s, r_s, a_s, store, field_of, per * group, group)
        else:
            for k in range(chips if not whole else 0):
                for s in range(per):
                    outs[0][k, s] = jnp.zeros((width, lanes), BF16)

            def store(i, u, at, out):
                f = i * group + u
                slot = f if whole else place_ref[f]
                outs[0][lax.div(slot, per), lax.rem(slot, per), at : at + size, :] = out

            attend(q_s, k_s, v_s, r_s, a_s, store, in_order, fields, group)


def interact(place, given, chips, weights, fields):
    per, width, lanes = given[0].shape[-3:]
    group = divisor(math.gcd(fields, chips), (4, 2, 1))
    wide = pltpu.VMEM((fields, width, lanes), F32)
    vmem = pl.BlockSpec(memory_space=pltpu.VMEM)
    scratch = [
        wide,
        pltpu.VMEM((width * fields, lanes), F32),
        pltpu.VMEM((width // 2, 2 * fields, lanes), BF16),
        pltpu.VMEM((fields // 2, 2 * width, lanes), BF16),
        wide,
        pltpu.VMEM((group * fields, lanes), F32),
        pltpu.VMEM((chips * per, width, lanes), BF16),
        pltpu.VMEM((fields, width, lanes), BF16),
    ]
    return pl.pallas_call(
        functools.partial(interact_kernel, chips=chips, group=group, fields=fields),
        out_shape=[jax.ShapeDtypeStruct(x.shape, BF16) for x in given],
        in_specs=[pl.BlockSpec(memory_space=pltpu.SMEM)] + [vmem] * (4 + len(given)),
        out_specs=[vmem] * len(given),
        scratch_shapes=scratch,
        compiler_params=pltpu.CompilerParams(vmem_limit_bytes=INTERACT_BYTES),
        cost_estimate=pl.CostEstimate(
            flops=12_000_000_000, bytes_accessed=4_000_000, transcendentals=0
        ),
        name="interact",
    )(place, *weights, *given)


def logit_kernel(w_ref, *refs):
    blocks, o_ref = refs[:-1], refs[-1]
    per, width, lanes = blocks[0].shape
    total = jnp.zeros((ROWS, lanes), F32)
    for k, block in enumerate(blocks):
        rest = w_ref[k : k + 1, :]
        pieces = []
        for _ in range(3):
            piece = rest.astype(BF16)
            rest = rest - piece.astype(F32)
            pieces.append(piece.astype(F32))
        pieces.append(jnp.zeros((ROWS - 3, per * width), F32))
        left = jnp.concatenate(pieces, axis=0).astype(BF16)
        right = block[...].reshape(per * width, lanes)
        total = total + jnp.dot(left, right, preferred_element_type=F32)
    o_ref[...] = jnp.sum(total, axis=0, keepdims=True)


def logit(weight, blocks):
    lanes = blocks[0].shape[-1]
    vmem = pl.BlockSpec(memory_space=pltpu.VMEM)
    return pl.pallas_call(
        logit_kernel,
        out_shape=jax.ShapeDtypeStruct((1, lanes), F32),
        in_specs=[vmem] * (1 + len(blocks)),
        out_specs=vmem,
        compiler_params=pltpu.CompilerParams(vmem_limit_bytes=SMALL_BYTES),
        cost_estimate=pl.CostEstimate(
            flops=1_000_000_000, bytes_accessed=1_000_000, transcendentals=0
        ),
        name="logit",
    )(weight, *blocks)


def per_device(
    feature_ids,
    field_slot,
    table,
    query_weight,
    key_weight,
    value_weight,
    residual_weight,
    out_weight,
):
    total, per = feature_ids.shape
    owned, width = table.shape
    chips = lax.axis_size("fld")
    reps = lax.axis_size("rep")
    half = total // reps
    peer = half // chips
    rows_slot = owned * reps // per
    slot_count = chips * per
    fields = field_slot.shape[0]

    spans = [(r * owned // rows_slot, -(-(r + 1) * owned // rows_slot)) for r in range(reps)]
    held = max(b - a for a, b in spans)
    held_slots = [[min(a, per - held) + j for j in range(held)] for a, _ in spans]
    sources = tuple(
        tuple((r, held_slots[r].index(s)) for r in range(reps) if spans[r][0] <= s < spans[r][1])
        for s in range(per)
    )
    step = divisor(owned, (16384, 8192, 4096, 2048, 1024, 512, 256))
    slot_ids = jnp.transpose(feature_ids)
    table_t = jnp.transpose(table)
    ranks = range(reps)

    def look_up(low, high):
        shift_of = [
            [(held_slots[r][j]) * rows_slot - r * owned for r in ranks] for j in range(low, high)
        ]
        starts = [max(0, shift_of[0][r]) // step for r in ranks]
        bounds_of = [starts] + [
            [max(starts[r], min(owned // step, -(-(shift[r] + rows_slot) // step))) for r in ranks]
            for shift in shift_of
        ]
        most = max(end - start for end, start in zip(bounds_of[-1], starts)) * step
        slot_of = [[held_slots[r][j] for r in ranks] for j in range(low, high)]
        return lookup(slot_ids, table_t, chips, slot_of, shift_of, bounds_of, step, most)

    found = look_up(0, held)
    found = [found[0]] + [
        lax.ppermute(found[n], "rep", [(r, (r + n) % reps) for r in ranks]) for n in range(1, reps)
    ]
    single = slot_count != fields or chips > 8
    blocks = pack(found, sources, single)

    def exchange(blocks):
        if single:
            return [lax.all_to_all(blocks[0], "fld", 0, 0, tiled=True)]
        return swap(blocks)

    weights = (query_weight, key_weight, value_weight, residual_weight)
    hidden = interact(field_slot, exchange(blocks), chips, weights, fields)
    sent = exchange(hidden)

    slots = jnp.arange(slot_count, dtype=jnp.int32)
    if not single:
        slots = (slots + lax.axis_index("fld") * per) % slot_count
    select = (field_slot[:, None] == slots[None, :]).astype(F32)
    slot_weight = jnp.einsum("fs,fd->sd", select, out_weight, precision=lax.Precision.HIGHEST)
    if single:
        logits = jnp.einsum(
            "csdn,csd->n",
            hidden[0].astype(F32),
            slot_weight.reshape(chips, per, width),
            precision=lax.Precision.HIGHEST,
        ).reshape(1, peer)
        joined = sent[0].transpose(1, 2, 0, 3).reshape(per, width, half)
    else:
        logits = logit(slot_weight.reshape(chips, per * width), hidden)
        joined = join(sent)
    return (jnp.transpose(joined, (0, 2, 1)), logits)


def solution(mesh):
    placed = (P("groups", "fld"), P(), P(("fld", "rep"), None), P(), P(), P(), P(), P())

    return jax.shard_map(
        per_device,
        mesh=mesh,
        in_specs=placed,
        out_specs=(P("fld", ("groups", "rep"), None), P("rep", ("groups", "fld"))),
        check_vma=False,
    )
```

```python
import functools
import math

import jax
import jax.numpy as jnp
from jax import lax
from jax.experimental import pallas as pl
from jax.experimental.pallas import tpu as pltpu
from jax.sharding import PartitionSpec as P


HEADS = 2
F32 = jnp.float32
BF16 = jnp.bfloat16
LANES = 128
VMEM_BYTES = 52 * 1024 * 1024
INTERACT_BYTES = 24 * 1024 * 1024
SMALL_BYTES = 8 * 1024 * 1024


def divisor(count, options):
    return next(c for c in options if count % c == 0)


def by_rep(options):
    rep = lax.axis_index("rep")
    found = jnp.int32(options[0])
    for r, option in enumerate(options[1:], 1):
        found = jnp.where(rep == r, jnp.int32(option), found)
    return found


def lookup_kernel(
    ids_ref, tab_ref, *refs, step, slot_of, shift_of, bounds_of, owned
):
    outs = refs[:-10]
    land, tab, stage, ids_s, lines, odd_ref, row_ref, sem, ids_sem, row_sem = refs[-10:]
    chips, slots, width, lanes = outs[0].shape
    reps = len(bounds_of[0])
    blocks = chips * reps
    chip = lax.axis_index("fld")
    rep = lax.axis_index("rep")
    buffers = land.shape[0]
    batch = stage.shape[0] // lanes
    spare = tab.shape[0] - 8
    bounds = [by_rep(b) for b in bounds_of]
    first, last = bounds[0], bounds[-1]
    pairs = step // (2 * lanes)

    def fetch(c):
        b = lax.rem(c, buffers)
        at = pl.ds(pl.multiple_of(c * step, step), step)
        return pltpu.make_async_copy(tab_ref.at[:, at], land.at[b], sem.at[b])

    for i in range(buffers):

        @pl.when(first + i < last)
        def _():
            fetch(first + i).start()

    ids_copy = pltpu.make_async_copy(ids_ref, ids_s, ids_sem)
    ids_copy.start()
    tab[pl.ds(spare, 8), :] = jnp.zeros((8, 2 * width), F32)
    ids_copy.wait()
    for j in range(slots):
        shift = by_rep(shift_of[j])
        for b in range(blocks):
            to_rep = lax.rem(rep + b // chips, reps)
            to_chip = lax.rem(chip + b % chips, chips)
            at = pl.ds(pl.multiple_of((to_rep * chips + to_chip) * lanes, lanes), lanes)
            rows = ids_s[slot_of[j][0] : slot_of[j][0] + 1, at]
            for r, slot in enumerate(slot_of[j][1:], 1):
                rows = jnp.where(rep == r, ids_s[slot : slot + 1, at], rows)
            rows = rows + shift
            here = (rows >= 0) & (rows < owned)
            rows = rows - first * step
            line = ((rows >> 8) << 7) | (rows & (lanes - 1))
            lines[pl.ds(j * blocks + b, 1), :] = jnp.where(here, line, spare)
            odd_ref[pl.ds(j * blocks + b, 1), :] = (rows >> 7) & 1
    rows_copy = pltpu.make_async_copy(lines, row_ref, row_sem)
    rows_copy.start()
    for j in range(slots):

        def chunk(c, carry):
            fetch(c).wait()
            b = lax.rem(c, buffers)

            def turn(p, carry):
                at = pl.multiple_of(p * (2 * lanes), 2 * lanes)
                two = jnp.concatenate(
                    [land[b, :, pl.ds(at, lanes)], land[b, :, pl.ds(at + lanes, lanes)]], axis=0
                )
                to = pl.multiple_of((c - first) * (step // 2) + p * lanes, lanes)
                tab[pl.ds(to, lanes), :] = two.T.astype(F32)
                return carry

            lax.fori_loop(0, pairs, turn, 0, unroll=min(pairs, 64))

            @pl.when(c + buffers < last)
            def _():
                fetch(c + buffers).start()

            return carry

        lax.fori_loop(bounds[j], bounds[j + 1], chunk, 0)
        if j == 0:
            rows_copy.wait()

        def some_blocks(i, carry, j=j, out_ref=None, ahead=0):
            def some(n, carry):
                at = j * blocks + ahead + i * batch + n
                to = n * lanes
                for u in range(lanes):
                    stage[pl.ds(to + u, 1), :] = tab[pl.ds(row_ref[at, u], 1), :]
                return carry

            lax.fori_loop(0, batch, some, 0)
            for g in range(batch):
                b = i * batch + g
                turned = stage[g * lanes : (g + 1) * lanes].astype(BF16).T.astype(F32)
                odd = odd_ref[pl.ds(j * blocks + ahead + b, 1), :] > 0
                out_ref[b, j] = jnp.where(odd, turned[width:], turned[:width]).astype(BF16)
            return carry

        for n, out_ref in enumerate(outs):
            here = functools.partial(some_blocks, out_ref=out_ref, ahead=n * chips)
            lax.fori_loop(0, chips // batch, here, 0)


def lookup(ids, table_t, chips, slot_of, shift_of, bounds_of, step, most):
    width, owned = table_t.shape
    slots = len(slot_of)
    buffers = min(4, owned // step)
    reps = len(bounds_of[0])
    blocks = chips * reps
    batch = divisor(chips, (4, 2, 1))
    vmem = pl.BlockSpec(memory_space=pltpu.VMEM)
    return pl.pallas_call(
        functools.partial(
            lookup_kernel,
            step=step,
            slot_of=slot_of,
            shift_of=shift_of,
            bounds_of=bounds_of,
            owned=owned,
        ),
        out_shape=[jax.ShapeDtypeStruct((chips, slots, width, LANES), BF16)] * reps,
        in_specs=[pl.BlockSpec(memory_space=pltpu.HBM)] * 2,
        out_specs=[vmem] * reps,
        scratch_shapes=[
            pltpu.VMEM((buffers, width, step), BF16),
            pltpu.VMEM((most // 2 + 8, 2 * width), F32),
            pltpu.VMEM((batch * LANES, 2 * width), F32),
            pltpu.VMEM(ids.shape, jnp.int32),
            pltpu.VMEM((slots * blocks, LANES), jnp.int32),
            pltpu.VMEM((slots * blocks, LANES), jnp.int32),
            pltpu.SMEM((slots * blocks, LANES), jnp.int32),
            pltpu.SemaphoreType.DMA((buffers,)),
            pltpu.SemaphoreType.DMA,
            pltpu.SemaphoreType.DMA,
        ],
        compiler_params=pltpu.CompilerParams(vmem_limit_bytes=VMEM_BYTES),
        cost_estimate=pl.CostEstimate(
            flops=slots * 12_000_000_000, bytes_accessed=2 * most * width, transcendentals=0
        ),
    )(ids, table_t)


def pack_kernel(*refs, sources, reps, chips):
    found, outs = refs[:reps], refs[reps:]
    rep = lax.axis_index("rep")
    chip = lax.axis_index("fld")
    for k in range(chips):
        for s, parts in enumerate(sources):
            total = None
            for r, j in parts:
                piece = found[0][k, j]
                for n in range(1, reps):
                    piece = jnp.where(lax.rem(rep + reps - n, reps) == r, found[n][k, j], piece)
                total = piece if total is None else total + piece
            if len(outs) == chips:
                outs[k][s] = total
            else:
                outs[0][lax.rem(chip + k, chips), s] = total


def pack(found, sources, single):
    reps = len(found)
    chips, _, width, lanes = found[0].shape
    per = len(sources)
    vmem = pl.BlockSpec(memory_space=pltpu.VMEM)
    block = jax.ShapeDtypeStruct((per, width, lanes), BF16)
    outs = [jax.ShapeDtypeStruct((chips, *block.shape), BF16)] if single else [block] * chips
    return pl.pallas_call(
        functools.partial(pack_kernel, sources=sources, reps=reps, chips=chips),
        out_shape=outs,
        in_specs=[vmem] * reps,
        out_specs=[vmem] * len(outs),
        compiler_params=pltpu.CompilerParams(vmem_limit_bytes=SMALL_BYTES),
        name="pack",
    )(*found)


def join_kernel(*refs):
    parts, out_ref, sem = refs[:-2], refs[-2], refs[-1]
    chips = len(parts)
    lanes = parts[0].shape[-1]
    chip = lax.axis_index("fld")
    copies = []
    for k, part in enumerate(parts):
        at = pl.multiple_of(lax.rem(chip + chips - k, chips) * lanes, lanes)
        copies.append(pltpu.make_async_copy(part, out_ref.at[:, :, pl.ds(at, lanes)], sem.at[k]))
    for copy in copies:
        copy.start()
    for copy in copies:
        copy.wait()


def join(parts):
    per, width, lanes = parts[0].shape
    anywhere = pl.BlockSpec(memory_space=pl.ANY)
    return pl.pallas_call(
        join_kernel,
        out_shape=jax.ShapeDtypeStruct((per, width, lanes * len(parts)), BF16),
        in_specs=[anywhere] * len(parts),
        out_specs=anywhere,
        scratch_shapes=[pltpu.SemaphoreType.DMA((len(parts),))],
        compiler_params=pltpu.CompilerParams(vmem_limit_bytes=SMALL_BYTES),
        name="join",
    )(*parts)


def swap(blocks):
    chips = len(blocks)
    out = [blocks[0]]
    for k in range(1, chips):
        route = [(i, (i + k) % chips) for i in range(chips)]
        out.append(lax.ppermute(blocks[k], "fld", route))
    return out


ROWS = 8
CHAINS = 4


def project(load, w, q_s, kt_s, k_s, v_s, r_s):
    fields, width, lanes = q_s.shape

    def pair(i, carry):
        f = 2 * i
        x2 = jnp.concatenate([load(f), load(f + 1)], axis=1)
        y = lax.dot_general(w, x2, (((1,), (0,)), ((), ())), preferred_element_type=F32)
        ys = [y[:, :lanes], y[:, lanes:]]
        for u in range(2):
            q_s[f + u] = ys[u][:width]
            kt_s[pl.ds(f + u, width, stride=fields), :] = ys[u][width : 2 * width]
            r_s[f + u] = ys[u][3 * width :]
        for t in range(width // ROWS):
            at = 2 * width + ROWS * t
            two = jnp.concatenate([yu[at : at + ROWS] for yu in ys], axis=0)
            v_s[i, 2 * ROWS * t : 2 * ROWS * (t + 1)] = two.astype(BF16)
        return carry

    lax.fori_loop(0, fields // 2, pair, 0, unroll=divisor(fields // 2, (10, 8, 5, 4, 2, 1)))

    def turn(i, carry):
        rows = [
            kt_s[pl.ds(pl.multiple_of((2 * i + u) * fields, ROWS), fields), :] for u in range(2)
        ]
        for t in range(fields // ROWS):
            two = jnp.concatenate([x[ROWS * t : ROWS * (t + 1)] for x in rows], axis=0)
            k_s[i, 2 * ROWS * t : 2 * ROWS * (t + 1)] = two.astype(BF16)
        return carry

    lax.fori_loop(0, width // 2, turn, 0, unroll=4)


def spread(a, b):
    shape = (ROWS, a.shape[1])
    two = jnp.concatenate([jnp.broadcast_to(a, shape), jnp.broadcast_to(b, shape)], axis=0)
    return two.astype(BF16).astype(F32)


def halves(x):
    return x[:ROWS] + x[ROWS:]


def attend(q_s, k_s, v_s, r_s, a_s, store, field_of, count, group):
    fields, width, _ = q_s.shape
    size = width // HEADS
    scale = math.log2(math.e) / math.sqrt(size)
    tiles = fields // ROWS
    whole = tiles // CHAINS * CHAINS
    jobs = [
        [(u, t) for t in range(n, n + CHAINS)] for n in range(0, whole, CHAINS) for u in range(group)
    ]
    left = [(u, t) for t in range(whole, tiles) for u in range(group)]
    jobs += [left[n : n + CHAINS] for n in range(0, len(left), CHAINS)]

    def some(i, carry):
        own = [field_of(i, u) for u in range(group)]
        for h in range(HEADS):
            scores = {}
            for job in jobs:
                sums = {}
                for d in range(h * size, (h + 1) * size, 2):
                    qs = {
                        u: spread(q_s[own[u], pl.ds(d, 1), :], q_s[own[u], pl.ds(d + 1, 1), :])
                        for u, _ in job
                    }
                    for u, t in job:
                        match = k_s[d // 2, 2 * ROWS * t : 2 * ROWS * (t + 1), :].astype(F32)
                        term = match * qs[u]
                        sums[u, t] = sums[u, t] + term if (u, t) in sums else term
                scores.update((key, halves(x)) for key, x in sums.items())
            for u in range(group):
                score = jnp.concatenate([scores[u, t] for t in range(tiles)], axis=0)
                top = jnp.max(score, axis=0, keepdims=True)
                e = jnp.exp2((score - top) * scale)
                a_s[u * fields : (u + 1) * fields, :] = e / jnp.sum(e, axis=0, keepdims=True)
            for u in range(group):
                sums = {}
                for g in range(0, fields, 2):
                    at = u * fields + g
                    weight = spread(a_s[at : at + 1, :], a_s[at + 1 : at + 2, :])
                    for t in range(h * size // ROWS, (h + 1) * size // ROWS):
                        content = v_s[g // 2, 2 * ROWS * t : 2 * ROWS * (t + 1), :].astype(F32)
                        term = content * weight
                        sums[t] = sums[t] + term if t in sums else term
                mixed = jnp.concatenate([halves(x) for x in sums.values()], axis=0)
                out = mixed + r_s[own[u], h * size : (h + 1) * size, :]
                store(i, u, h * size, jnp.maximum(out, 0.0).astype(BF16))
        return carry

    lax.fori_loop(0, count // group, some, 0)


def layer_weights(refs, l):
    return jnp.concatenate([ref[l].astype(F32).T.astype(BF16) for ref in refs], axis=0)


def shifts_of(chips, group):
    order = sorted(range(chips), key=lambda k: abs(k - chips / 2))
    groups = [order[n : n + group] for n in range(0, chips, group)]
    half = -(-len(groups) // 2)
    return groups[:half], groups[half:]


def last_layer(groups, outs, q_s, k_s, v_s, r_s, a_s, chips, group):
    per = outs[0].shape[0]
    size = outs[0].shape[1] // HEADS
    chip = lax.axis_index("fld")
    for n, ks in enumerate(groups):

        def field_of(i, u, ks=ks):
            return lax.rem(chip + ks[u], chips) * per + i

        def store(i, u, at, out, n=n):
            outs[n * group + u][i, at : at + size, :] = out

        attend(q_s, k_s, v_s, r_s, a_s, store, field_of, per * group, group)


def interact_kernel(place_ref, wq_ref, wk_ref, wv_ref, wr_ref, *refs, chips, group, fields, single):
    a_s, kt_s, x_s, h_s = refs[-4:]
    ins, outs, (q_s, k_s, v_s, r_s) = refs[: 1 if single else chips], refs[:-8], refs[-8:-4]
    outs = outs[len(ins) :]
    per, width, lanes = ins[0].shape[-3:]
    layers = wq_ref.shape[0]
    size = width // HEADS
    whole = chips * per == fields
    chip = lax.axis_index("fld")
    weights = (wq_ref, wk_ref, wv_ref, wr_ref)

    def in_order(i, u):
        return i * group + u

    for k in range(chips):
        back = lax.rem(chip + chips - k, chips)
        for s in range(per):
            x_s[back * per + s] = ins[0][back, s] if single else ins[k][s]

    for l in range(layers):
        if l == 0:
            load = lambda f: x_s[f if whole else place_ref[f]]
        else:
            load = lambda f: h_s[f]
        project(load, layer_weights(weights, l), q_s, kt_s, k_s, v_s, r_s)
        if l < layers - 1:

            def store(i, u, at, out):
                h_s[i * group + u, at : at + size, :] = out

            attend(q_s, k_s, v_s, r_s, a_s, store, in_order, fields, group)
        elif not single:
            groups = shifts_of(chips, group)[0]
            last_layer(groups, outs, q_s, k_s, v_s, r_s, a_s, chips, group)
        else:
            for k in range(chips if not whole else 0):
                for s in range(per):
                    outs[0][k, s] = jnp.zeros((width, lanes), BF16)

            def store(i, u, at, out):
                f = i * group + u
                slot = f if whole else place_ref[f]
                outs[0][lax.div(slot, per), lax.rem(slot, per), at : at + size, :] = out

            attend(q_s, k_s, v_s, r_s, a_s, store, in_order, fields, group)


def rest_kernel(q_s, k_s, v_s, r_s, *refs, chips, group):
    groups = shifts_of(chips, group)[1]
    last_layer(groups, refs[:-1], q_s, k_s, v_s, r_s, refs[-1], chips, group)


def interact(place, given, chips, weights, fields, single):
    per, width, lanes = given[0].shape[-3:]
    group = divisor(math.gcd(fields, chips), (4, 2, 1))
    vmem = pl.BlockSpec(memory_space=pltpu.VMEM)
    wide = ((fields, width, lanes), F32)
    state = [
        wide,
        ((width // 2, 2 * fields, lanes), BF16),
        ((fields // 2, 2 * width, lanes), BF16),
        wide,
    ]
    attention = pltpu.VMEM((group * fields, lanes), F32)
    scratch = [
        attention,
        pltpu.VMEM((width * fields, lanes), F32),
        pltpu.VMEM((chips * per, width, lanes), BF16),
        pltpu.VMEM((fields, width, lanes), BF16),
    ]
    first, second = ([], []) if single else shifts_of(chips, group)
    first, second = sum(first, []), sum(second, [])
    made = [jax.ShapeDtypeStruct(given[0].shape, BF16)] * (1 if single else len(first))
    if second:
        made = made + [jax.ShapeDtypeStruct(*x) for x in state]
    else:
        scratch = [pltpu.VMEM(*x) for x in state] + scratch
    done = pl.pallas_call(
        functools.partial(
            interact_kernel, chips=chips, group=group, fields=fields, single=single
        ),
        out_shape=made,
        in_specs=[pl.BlockSpec(memory_space=pltpu.SMEM)] + [vmem] * (4 + len(given)),
        out_specs=[vmem] * len(made),
        scratch_shapes=scratch,
        compiler_params=pltpu.CompilerParams(vmem_limit_bytes=INTERACT_BYTES),
        cost_estimate=pl.CostEstimate(
            flops=12_000_000_000, bytes_accessed=4_000_000, transcendentals=0
        ),
        name="interact",
    )(place, *weights, *given)
    if single:
        return list(done), ()
    blocks = dict(zip(first, done))
    if second:
        made = [jax.ShapeDtypeStruct(given[0].shape, BF16)] * len(second)
        rest = pl.pallas_call(
            functools.partial(rest_kernel, chips=chips, group=group),
            out_shape=made,
            in_specs=[vmem] * len(state),
            out_specs=[vmem] * len(made),
            scratch_shapes=[attention],
            compiler_params=pltpu.CompilerParams(vmem_limit_bytes=INTERACT_BYTES),
            cost_estimate=pl.CostEstimate(
                flops=3_000_000_000, bytes_accessed=4_000_000, transcendentals=0
            ),
            name="rest",
        )(*done[len(first) :])
        blocks.update(zip(second, rest))
    return [blocks[k] for k in range(chips)], first if second else ()


def logit_kernel(w_ref, *refs):
    blocks, o_ref = refs[:-1], refs[-1]
    per, width, lanes = blocks[0].shape
    total = jnp.zeros((ROWS, lanes), F32)
    for k, block in enumerate(blocks):
        rest = w_ref[k : k + 1, :]
        pieces = []
        for _ in range(3):
            piece = rest.astype(BF16)
            rest = rest - piece.astype(F32)
            pieces.append(piece.astype(F32))
        pieces.append(jnp.zeros((ROWS - 3, per * width), F32))
        left = jnp.concatenate(pieces, axis=0).astype(BF16)
        right = block[...].reshape(per * width, lanes)
        total = total + jnp.dot(left, right, preferred_element_type=F32)
    o_ref[...] = jnp.sum(total, axis=0, keepdims=True)


def logit(weight, blocks):
    lanes = blocks[0].shape[-1]
    vmem = pl.BlockSpec(memory_space=pltpu.VMEM)
    return pl.pallas_call(
        logit_kernel,
        out_shape=jax.ShapeDtypeStruct((1, lanes), F32),
        in_specs=[vmem] * (1 + len(blocks)),
        out_specs=vmem,
        compiler_params=pltpu.CompilerParams(vmem_limit_bytes=SMALL_BYTES),
        cost_estimate=pl.CostEstimate(
            flops=1_000_000_000, bytes_accessed=1_000_000, transcendentals=0
        ),
        name="logit",
    )(weight, *blocks)


def per_device(
    feature_ids,
    field_slot,
    table,
    query_weight,
    key_weight,
    value_weight,
    residual_weight,
    out_weight,
):
    total, per = feature_ids.shape
    owned, width = table.shape
    chips = lax.axis_size("fld")
    reps = lax.axis_size("rep")
    half = total // reps
    peer = half // chips
    rows_slot = owned * reps // per
    slot_count = chips * per
    fields = field_slot.shape[0]

    spans = [(r * owned // rows_slot, -(-(r + 1) * owned // rows_slot)) for r in range(reps)]
    held = max(b - a for a, b in spans)
    held_slots = [[min(a, per - held) + j for j in range(held)] for a, _ in spans]
    sources = tuple(
        tuple((r, held_slots[r].index(s)) for r in range(reps) if spans[r][0] <= s < spans[r][1])
        for s in range(per)
    )
    step = divisor(owned, (16384, 8192, 4096, 2048, 1024, 512, 256))
    slot_ids = jnp.transpose(feature_ids)
    table_t = jnp.transpose(table)
    ranks = range(reps)

    def look_up(low, high):
        shift_of = [
            [(held_slots[r][j]) * rows_slot - r * owned for r in ranks] for j in range(low, high)
        ]
        starts = [max(0, shift_of[0][r]) // step for r in ranks]
        bounds_of = [starts] + [
            [max(starts[r], min(owned // step, -(-(shift[r] + rows_slot) // step))) for r in ranks]
            for shift in shift_of
        ]
        most = max(end - start for end, start in zip(bounds_of[-1], starts)) * step
        slot_of = [[held_slots[r][j] for r in ranks] for j in range(low, high)]
        return lookup(slot_ids, table_t, chips, slot_of, shift_of, bounds_of, step, most)

    found = look_up(0, held)
    found = [found[0]] + [
        lax.ppermute(found[n], "rep", [(r, (r + n) % reps) for r in ranks]) for n in range(1, reps)
    ]
    single = slot_count != fields or chips > 8
    blocks = pack(found, sources, single)

    def exchange(blocks):
        if single:
            return [lax.all_to_all(blocks[0], "fld", 0, 0, tiled=True)]
        return swap(blocks)

    weights = (query_weight, key_weight, value_weight, residual_weight)
    hidden, _ = interact(field_slot, exchange(blocks), chips, weights, fields, single)
    sent = exchange(hidden)

    slots = jnp.arange(slot_count, dtype=jnp.int32)
    if not single:
        slots = (slots + lax.axis_index("fld") * per) % slot_count
    select = (field_slot[:, None] == slots[None, :]).astype(F32)
    slot_weight = jnp.einsum("fs,fd->sd", select, out_weight, precision=lax.Precision.HIGHEST)
    if single:
        logits = jnp.einsum(
            "csdn,csd->n",
            hidden[0].astype(F32),
            slot_weight.reshape(chips, per, width),
            precision=lax.Precision.HIGHEST,
        ).reshape(1, peer)
        joined = sent[0].transpose(1, 2, 0, 3).reshape(per, width, half)
    else:
        logits = logit(slot_weight.reshape(chips, per * width), hidden)
        joined = join(sent)
    return (jnp.transpose(joined, (0, 2, 1)), logits)


def solution(mesh):
    placed = (P("groups", "fld"), P(), P(("fld", "rep"), None), P(), P(), P(), P(), P())

    return jax.shard_map(
        per_device,
        mesh=mesh,
        in_specs=placed,
        out_specs=(P("fld", ("groups", "rep"), None), P("rep", ("groups", "fld"))),
        check_vma=False,
    )
```

```python
import functools
import math

import jax
import jax.numpy as jnp
from jax import lax
from jax.experimental import pallas as pl
from jax.experimental.pallas import tpu as pltpu
from jax.sharding import PartitionSpec as P

HEADS = 2
F32 = jnp.float32
BF16 = jnp.bfloat16
LANES = 128
VMEM_BYTES = 52 * 1024 * 1024
INTERACT_BYTES = 24 * 1024 * 1024
SMALL_BYTES = 8 * 1024 * 1024


def divisor(count, options):
    return next(c for c in options if count % c == 0)


def by_rep(options):
    rep = lax.axis_index("rep")
    found = jnp.int32(options[0])
    for r, option in enumerate(options[1:], 1):
        found = jnp.where(rep == r, jnp.int32(option), found)
    return found


def lookup_kernel(
    ids_ref, tab_ref, *refs, step, slot_of, shift_of, bounds_of, owned
):
    outs = refs[:-8]
    land, tab, stage, lines, odd_ref, row_ref, sem, row_sem = refs[-8:]
    chips, slots, width, lanes = outs[0].shape
    reps = len(bounds_of[0])
    blocks = chips * reps
    chip = lax.axis_index("fld")
    rep = lax.axis_index("rep")
    buffers = land.shape[0]
    batch = stage.shape[0] // lanes
    spare = tab.shape[0] - 8
    bounds = [by_rep(b) for b in bounds_of]
    first, last = bounds[0], bounds[-1]
    pairs = step // (2 * lanes)

    def fetch(c):
        b = lax.rem(c, buffers)
        at = pl.ds(pl.multiple_of(c * step, step), step)
        return pltpu.make_async_copy(tab_ref.at[:, at], land.at[b], sem.at[b])

    for i in range(buffers):

        @pl.when(first + i < last)
        def _():
            fetch(first + i).start()

    tab[pl.ds(spare, 8), :] = jnp.zeros((8, 2 * width), F32)
    for j in range(slots):
        shift = by_rep(shift_of[j])
        for b in range(blocks):
            to_rep = lax.rem(rep + b // chips, reps)
            to_chip = lax.rem(chip + b % chips, chips)
            at = pl.ds(pl.multiple_of((to_rep * chips + to_chip) * lanes, lanes), lanes)
            rows = ids_ref[slot_of[j][0] : slot_of[j][0] + 1, at]
            for r, slot in enumerate(slot_of[j][1:], 1):
                rows = jnp.where(rep == r, ids_ref[slot : slot + 1, at], rows)
            rows = rows + shift
            here = (rows >= 0) & (rows < owned)
            rows = rows - first * step
            line = ((rows >> 8) << 7) | (rows & (lanes - 1))
            lines[pl.ds(j * blocks + b, 1), :] = jnp.where(here, line, spare)
            odd_ref[pl.ds(j * blocks + b, 1), :] = (rows >> 7) & 1
    rows_copy = pltpu.make_async_copy(lines, row_ref, row_sem)
    rows_copy.start()
    for j in range(slots):

        def chunk(c, carry):
            fetch(c).wait()
            b = lax.rem(c, buffers)

            def turn(p, carry):
                at = pl.multiple_of(p * (2 * lanes), 2 * lanes)
                two = jnp.concatenate(
                    [land[b, :, pl.ds(at, lanes)], land[b, :, pl.ds(at + lanes, lanes)]], axis=0
                )
                to = pl.multiple_of((c - first) * (step // 2) + p * lanes, lanes)
                tab[pl.ds(to, lanes), :] = two.T.astype(F32)
                return carry

            lax.fori_loop(0, pairs, turn, 0, unroll=min(pairs, 64))

            @pl.when(c + buffers < last)
            def _():
                fetch(c + buffers).start()

            return carry

        lax.fori_loop(bounds[j], bounds[j + 1], chunk, 0)
        if j == 0:
            rows_copy.wait()

        def some_blocks(i, carry, j=j, out_ref=None, ahead=0):
            def some(n, carry):
                at = j * blocks + ahead + i * batch + n
                to = n * lanes
                for u in range(lanes):
                    stage[pl.ds(to + u, 1), :] = tab[pl.ds(row_ref[at, u], 1), :]
                return carry

            lax.fori_loop(0, batch, some, 0)
            for g in range(batch):
                b = i * batch + g
                turned = stage[g * lanes : (g + 1) * lanes].astype(BF16).T.astype(F32)
                odd = odd_ref[pl.ds(j * blocks + ahead + b, 1), :] > 0
                out_ref[b, j] = jnp.where(odd, turned[width:], turned[:width]).astype(BF16)
            return carry

        for n, out_ref in enumerate(outs):
            here = functools.partial(some_blocks, out_ref=out_ref, ahead=n * chips)
            lax.fori_loop(0, chips // batch, here, 0)


def lookup(ids, table_t, chips, slot_of, shift_of, bounds_of, step, most):
    width, owned = table_t.shape
    slots = len(slot_of)
    buffers = min(4, owned // step)
    reps = len(bounds_of[0])
    blocks = chips * reps
    batch = divisor(chips, (8, 4, 2, 1))
    vmem = pl.BlockSpec(memory_space=pltpu.VMEM)
    anywhere = pl.BlockSpec(memory_space=pl.ANY)
    return pl.pallas_call(
        functools.partial(
            lookup_kernel,
            step=step,
            slot_of=slot_of,
            shift_of=shift_of,
            bounds_of=bounds_of,
            owned=owned,
        ),
        out_shape=[jax.ShapeDtypeStruct((chips, slots, width, LANES), BF16)] * reps,
        in_specs=[vmem, anywhere],
        out_specs=[vmem] * reps,
        scratch_shapes=[
            pltpu.VMEM((buffers, width, step), BF16),
            pltpu.VMEM((most // 2 + 8, 2 * width), F32),
            pltpu.VMEM((batch * LANES, 2 * width), F32),
            pltpu.VMEM((slots * blocks, LANES), jnp.int32),
            pltpu.VMEM((slots * blocks, LANES), jnp.int32),
            pltpu.SMEM((slots * blocks, LANES), jnp.int32),
            pltpu.SemaphoreType.DMA((buffers,)),
            pltpu.SemaphoreType.DMA,
        ],
        compiler_params=pltpu.CompilerParams(vmem_limit_bytes=VMEM_BYTES),
        cost_estimate=pl.CostEstimate(
            flops=slots * 12_000_000_000, bytes_accessed=2 * most * width, transcendentals=0
        ),
    )(ids, table_t)


def pack_kernel(*refs, sources, reps, chips):
    found, outs = refs[:reps], refs[reps:]
    rep = lax.axis_index("rep")
    chip = lax.axis_index("fld")
    for k in range(chips):
        for s, parts in enumerate(sources):
            total = None
            for r, j in parts:
                piece = found[0][k, j]
                for n in range(1, reps):
                    piece = jnp.where(lax.rem(rep + reps - n, reps) == r, found[n][k, j], piece)
                total = piece if total is None else total + piece
            if len(outs) == chips:
                outs[k][s] = total
            else:
                outs[0][lax.rem(chip + k, chips), s] = total


def pack(found, sources, single):
    reps = len(found)
    chips, _, width, lanes = found[0].shape
    per = len(sources)
    vmem = pl.BlockSpec(memory_space=pltpu.VMEM)
    block = jax.ShapeDtypeStruct((per, width, lanes), BF16)
    outs = [jax.ShapeDtypeStruct((chips, *block.shape), BF16)] if single else [block] * chips
    return pl.pallas_call(
        functools.partial(pack_kernel, sources=sources, reps=reps, chips=chips),
        out_shape=outs,
        in_specs=[vmem] * reps,
        out_specs=[vmem] * len(outs),
        compiler_params=pltpu.CompilerParams(vmem_limit_bytes=SMALL_BYTES),
        name="pack",
    )(*found)


def join_kernel(*refs):
    parts, out_ref, sem = refs[:-2], refs[-2], refs[-1]
    chips = len(parts)
    lanes = parts[0].shape[-1]
    chip = lax.axis_index("fld")
    copies = []
    for k, part in enumerate(parts):
        at = pl.multiple_of(lax.rem(chip + chips - k, chips) * lanes, lanes)
        copies.append(pltpu.make_async_copy(part, out_ref.at[:, :, pl.ds(at, lanes)], sem.at[k]))
    for copy in copies:
        copy.start()
    for copy in copies:
        copy.wait()


def join(parts):
    per, width, lanes = parts[0].shape
    anywhere = pl.BlockSpec(memory_space=pl.ANY)
    return pl.pallas_call(
        join_kernel,
        out_shape=jax.ShapeDtypeStruct((per, width, lanes * len(parts)), BF16),
        in_specs=[anywhere] * len(parts),
        out_specs=anywhere,
        scratch_shapes=[pltpu.SemaphoreType.DMA((len(parts),))],
        compiler_params=pltpu.CompilerParams(vmem_limit_bytes=SMALL_BYTES),
        name="join",
    )(*parts)


def swap(blocks):
    chips = len(blocks)
    out = [blocks[0]]
    for k in range(1, chips):
        out.append(lax.ppermute(blocks[k], "fld", [(i, (i + k) % chips) for i in range(chips)]))
    return out


ROWS = 8
CHAINS = 4


def project(load, w, q_s, kt_s, k_s, v_s, r_s):
    fields, width, lanes = q_s.shape

    def pair(i, carry):
        f = 2 * i
        x2 = jnp.concatenate([load(f), load(f + 1)], axis=1)
        y = lax.dot_general(w, x2, (((1,), (0,)), ((), ())), preferred_element_type=F32)
        ys = [y[:, :lanes], y[:, lanes:]]
        for u in range(2):
            q_s[f + u] = ys[u][:width]
            kt_s[pl.ds(f + u, width, stride=fields), :] = ys[u][width : 2 * width]
            r_s[f + u] = ys[u][3 * width :]
        for t in range(width // ROWS):
            at = 2 * width + ROWS * t
            two = jnp.concatenate([yu[at : at + ROWS] for yu in ys], axis=0)
            v_s[i, 2 * ROWS * t : 2 * ROWS * (t + 1)] = two.astype(BF16)
        return carry

    lax.fori_loop(0, fields // 2, pair, 0, unroll=divisor(fields // 2, (20, 10, 8, 5, 4, 2, 1)))

    def turn(i, carry):
        rows = [
            kt_s[pl.ds(pl.multiple_of((2 * i + u) * fields, ROWS), fields), :] for u in range(2)
        ]
        for t in range(fields // ROWS):
            two = jnp.concatenate([x[ROWS * t : ROWS * (t + 1)] for x in rows], axis=0)
            k_s[i, 2 * ROWS * t : 2 * ROWS * (t + 1)] = two.astype(BF16)
        return carry

    lax.fori_loop(0, width // 2, turn, 0, unroll=4)


def spread(a, b):
    shape = (ROWS, a.shape[1])
    two = jnp.concatenate([jnp.broadcast_to(a, shape), jnp.broadcast_to(b, shape)], axis=0)
    return two.astype(BF16).astype(F32)


def halves(x):
    return x[:ROWS] + x[ROWS:]


def attend(q_s, k_s, v_s, r_s, a_s, store, field_of, count, group):
    fields, width, _ = q_s.shape
    size = width // HEADS
    scale = math.log2(math.e) / math.sqrt(size)
    tiles = fields // ROWS
    whole = tiles // CHAINS * CHAINS
    jobs = [
        [(u, t) for t in range(n, n + CHAINS)] for n in range(0, whole, CHAINS) for u in range(group)
    ]
    left = [(u, t) for t in range(whole, tiles) for u in range(group)]
    jobs += [left[n : n + CHAINS] for n in range(0, len(left), CHAINS)]

    def some(i, carry):
        own = [field_of(i, u) for u in range(group)]
        for h in range(HEADS):
            scores = {}
            for job in jobs:
                sums = {}
                for d in range(h * size, (h + 1) * size, 2):
                    qs = {
                        u: spread(q_s[own[u], pl.ds(d, 1), :], q_s[own[u], pl.ds(d + 1, 1), :])
                        for u, _ in job
                    }
                    for u, t in job:
                        match = k_s[d // 2, 2 * ROWS * t : 2 * ROWS * (t + 1), :].astype(F32)
                        term = match * qs[u]
                        sums[u, t] = sums[u, t] + term if (u, t) in sums else term
                scores.update((key, halves(x)) for key, x in sums.items())
            for u in range(group):
                score = jnp.concatenate([scores[u, t] for t in range(tiles)], axis=0)
                top = jnp.max(score, axis=0, keepdims=True)
                e = jnp.exp2((score - top) * scale)
                a_s[u * fields : (u + 1) * fields, :] = e / jnp.sum(e, axis=0, keepdims=True)
            for u in range(group):
                sums = {}
                for g in range(0, fields, 2):
                    at = u * fields + g
                    weight = spread(a_s[at : at + 1, :], a_s[at + 1 : at + 2, :])
                    for t in range(h * size // ROWS, (h + 1) * size // ROWS):
                        content = v_s[g // 2, 2 * ROWS * t : 2 * ROWS * (t + 1), :].astype(F32)
                        term = content * weight
                        sums[t] = sums[t] + term if t in sums else term
                mixed = jnp.concatenate([halves(x) for x in sums.values()], axis=0)
                out = mixed + r_s[own[u], h * size : (h + 1) * size, :]
                store(i, u, h * size, jnp.maximum(out, 0.0).astype(BF16))
        return carry

    lax.fori_loop(0, count // group, some, 0)


def layer_weights(refs, l):
    return jnp.concatenate([ref[l].astype(F32).T.astype(BF16) for ref in refs], axis=0)


def interact_kernel(place_ref, wq_ref, wk_ref, wv_ref, wr_ref, *refs, chips, group, fields):
    q_s, kt_s, k_s, v_s, r_s, a_s, x_s, h_s = refs[-8:]
    blocks = (len(refs) - 8) // 2
    ins, outs = refs[:blocks], refs[blocks : 2 * blocks]
    per, width, lanes = ins[0].shape[-3:]
    layers = wq_ref.shape[0]
    size = width // HEADS
    whole = chips * per == fields
    chip = lax.axis_index("fld")
    weights = (wq_ref, wk_ref, wv_ref, wr_ref)

    def in_order(i, u):
        return i * group + u

    for k in range(chips):
        back = lax.rem(chip + chips - k, chips)
        for s in range(per):
            x_s[back * per + s] = ins[k][s] if blocks == chips else ins[0][back, s]

    for l in range(layers):
        if l == 0:
            load = lambda f: x_s[f if whole else place_ref[f]]
        else:
            load = lambda f: h_s[f]
        project(load, layer_weights(weights, l), q_s, kt_s, k_s, v_s, r_s)
        if l < layers - 1:

            def store(i, u, at, out):
                h_s[i * group + u, at : at + size, :] = out

            attend(q_s, k_s, v_s, r_s, a_s, store, in_order, fields, group)
        elif blocks == chips:
            for low in range(0, chips, group):

                def field_of(i, u, low=low):
                    return lax.rem(chip + low + u, chips) * per + i

                def store(i, u, at, out, low=low):
                    outs[low + u][i, at : at + size, :] = out

                attend(q_s, k_s, v_s, r_s, a_s, store, field_of, per * group, group)
        else:
            for k in range(chips if not whole else 0):
                for s in range(per):
                    outs[0][k, s] = jnp.zeros((width, lanes), BF16)

            def store(i, u, at, out):
                f = i * group + u
                slot = f if whole else place_ref[f]
                outs[0][lax.div(slot, per), lax.rem(slot, per), at : at + size, :] = out

            attend(q_s, k_s, v_s, r_s, a_s, store, in_order, fields, group)


def interact(place, given, chips, weights, fields):
    per, width, lanes = given[0].shape[-3:]
    group = divisor(math.gcd(fields, chips), (8, 4, 2, 1))
    wide = pltpu.VMEM((fields, width, lanes), F32)
    vmem = pl.BlockSpec(memory_space=pltpu.VMEM)
    scratch = [
        wide,
        pltpu.VMEM((width * fields, lanes), F32),
        pltpu.VMEM((width // 2, 2 * fields, lanes), BF16),
        pltpu.VMEM((fields // 2, 2 * width, lanes), BF16),
        wide,
        pltpu.VMEM((group * fields, lanes), F32),
        pltpu.VMEM((chips * per, width, lanes), BF16),
        pltpu.VMEM((fields, width, lanes), BF16),
    ]
    return pl.pallas_call(
        functools.partial(interact_kernel, chips=chips, group=group, fields=fields),
        out_shape=[jax.ShapeDtypeStruct(x.shape, BF16) for x in given],
        in_specs=[pl.BlockSpec(memory_space=pltpu.SMEM)] + [vmem] * (4 + len(given)),
        out_specs=[vmem] * len(given),
        scratch_shapes=scratch,
        compiler_params=pltpu.CompilerParams(vmem_limit_bytes=INTERACT_BYTES),
        cost_estimate=pl.CostEstimate(
            flops=12_000_000_000, bytes_accessed=4_000_000, transcendentals=0
        ),
        name="interact",
    )(place, *weights, *given)


def logit_kernel(w_ref, *refs):
    blocks, o_ref = refs[:-1], refs[-1]
    per, width, lanes = blocks[0].shape
    total = jnp.zeros((ROWS, lanes), F32)
    for k, block in enumerate(blocks):
        rest = w_ref[k : k + 1, :]
        pieces = []
        for _ in range(3):
            piece = rest.astype(BF16)
            rest = rest - piece.astype(F32)
            pieces.append(piece.astype(F32))
        pieces.append(jnp.zeros((ROWS - 3, per * width), F32))
        left = jnp.concatenate(pieces, axis=0).astype(BF16)
        right = block[...].reshape(per * width, lanes)
        total = total + jnp.dot(left, right, preferred_element_type=F32)
    o_ref[...] = jnp.sum(total, axis=0, keepdims=True)


def logit(weight, blocks):
    lanes = blocks[0].shape[-1]
    vmem = pl.BlockSpec(memory_space=pltpu.VMEM)
    return pl.pallas_call(
        logit_kernel,
        out_shape=jax.ShapeDtypeStruct((1, lanes), F32),
        in_specs=[vmem] * (1 + len(blocks)),
        out_specs=vmem,
        compiler_params=pltpu.CompilerParams(vmem_limit_bytes=SMALL_BYTES),
        cost_estimate=pl.CostEstimate(
            flops=1_000_000_000, bytes_accessed=1_000_000, transcendentals=0
        ),
        name="logit",
    )(weight, *blocks)


def per_device(
    feature_ids,
    field_slot,
    table,
    query_weight,
    key_weight,
    value_weight,
    residual_weight,
    out_weight,
):
    total, per = feature_ids.shape
    owned, width = table.shape
    chips = lax.axis_size("fld")
    reps = lax.axis_size("rep")
    half = total // reps
    peer = half // chips
    rows_slot = owned * reps // per
    slot_count = chips * per
    fields = field_slot.shape[0]

    spans = [(r * owned // rows_slot, -(-(r + 1) * owned // rows_slot)) for r in range(reps)]
    held = max(b - a for a, b in spans)
    held_slots = [[min(a, per - held) + j for j in range(held)] for a, _ in spans]
    sources = tuple(
        tuple((r, held_slots[r].index(s)) for r in range(reps) if spans[r][0] <= s < spans[r][1])
        for s in range(per)
    )
    step = divisor(owned, (16384, 8192, 4096, 2048, 1024, 512, 256))
    slot_ids = jnp.transpose(feature_ids)
    table_t = jnp.transpose(table)
    ranks = range(reps)

    def look_up(low, high):
        shift_of = [
            [(held_slots[r][j]) * rows_slot - r * owned for r in ranks] for j in range(low, high)
        ]
        starts = [max(0, shift_of[0][r]) // step for r in ranks]
        bounds_of = [starts] + [
            [max(starts[r], min(owned // step, -(-(shift[r] + rows_slot) // step))) for r in ranks]
            for shift in shift_of
        ]
        most = max(end - start for end, start in zip(bounds_of[-1], starts)) * step
        slot_of = [[held_slots[r][j] for r in ranks] for j in range(low, high)]
        return lookup(slot_ids, table_t, chips, slot_of, shift_of, bounds_of, step, most)

    found = look_up(0, held)
    found = [found[0]] + [
        lax.ppermute(found[n], "rep", [(r, (r + n) % reps) for r in ranks]) for n in range(1, reps)
    ]
    single = slot_count != fields or chips > 8
    blocks = pack(found, sources, single)

    def exchange(blocks):
        if single:
            return [lax.all_to_all(blocks[0], "fld", 0, 0, tiled=True)]
        return swap(blocks)

    weights = (query_weight, key_weight, value_weight, residual_weight)
    hidden = interact(field_slot, exchange(blocks), chips, weights, fields)
    sent = exchange(hidden)

    slots = jnp.arange(slot_count, dtype=jnp.int32)
    if not single:
        slots = (slots + lax.axis_index("fld") * per) % slot_count
    select = (field_slot[:, None] == slots[None, :]).astype(F32)
    slot_weight = jnp.einsum("fs,fd->sd", select, out_weight, precision=lax.Precision.HIGHEST)
    if single:
        logits = jnp.einsum(
            "csdn,csd->n",
            hidden[0].astype(F32),
            slot_weight.reshape(chips, per, width),
            precision=lax.Precision.HIGHEST,
        ).reshape(1, peer)
        joined = sent[0].transpose(1, 2, 0, 3).reshape(per, width, half)
    else:
        logits = logit(slot_weight.reshape(chips, per * width), hidden)
        joined = join(sent)
    return (jnp.transpose(joined, (0, 2, 1)), logits)


def solution(mesh):
    placed = (P("groups", "fld"), P(), P(("fld", "rep"), None), P(), P(), P(), P(), P())

    return jax.shard_map(
        per_device,
        mesh=mesh,
        in_specs=placed,
        out_specs=(P("fld", ("groups", "rep"), None), P("rep", ("groups", "fld"))),
        check_vma=False,
    )
```
